32 devices in a mesh: groups: 2 (over x), seq: 16 (over z, y, core).
Axes of the slice: x: 2, y: 2, z: 4, core: 2. Of those that a mesh axis runs over, the one named last changes fastest.
Arguments:
- query_rows: bfloat16 [16384, 1536], P(('groups', 'seq')), parts along dimension 0, may hold values from -200 to 200
- key_rows: bfloat16 [16384, 1536], P(('groups', 'seq')), parts along dimension 0, may hold values from -6 to 6
- value_rows: bfloat16 [16384, 1536], P(('groups', 'seq')), parts along dimension 0, may hold values from -6 to 6
- select: int32 [64, 6], P('groups'), parts along dimension 0, may hold values from 0 to 31, as said below
- counts: int32 [64], P('groups'), parts along dimension 0, may hold values from 2 to 6, as said below
- guide_scale: float32 [2], P('groups'), parts along dimension 0, may hold values from 4 to 8
Outputs:
- guided: bfloat16 [8192, 1536], P(('groups', 'seq')), parts along dimension 0
The draws below stay inside these ranges and needn't reach their ends.
There are 2 independent parts, one for each index of `groups`. The reference program is written for one: setup_inputs(seed, part) draws one part's arguments, and reference() takes and returns one part's arrays. A program takes and returns all parts, laid end to end along the dimension named above; each array names one. Nothing has to cross between parts.
Inputs may be any that keep to these rules, and one draw needn't show every extreme that they name: Row i begins with i itself. Its first counts[i] entries are distinct and name tiles of shards within 2 of tile i's shard, where tile t belongs to shard t // 4. The query tiles of one shard select at most 2 distinct tiles of any one other shard, and every shard selects 2 tiles of each shard within 2 in every draw. Entries past counts[i] are valid tile numbers that are not used. `counts`: whole shards are heavy or light, so the work of one device differs by about two times between devices.
All inputs are finite; a program needn't handle non-finite values.
Results may differ from the reference program's by a relative error of at most 0.0075.
Values may be sent and summed in bfloat16 or wider, within the bound.
A program may use at most 128 MiB of HBM per device.

```python
import jax
import jax.numpy as jnp
from jax import lax

HEADS = 12
HEAD_DIM = 128
TILE = 128
TOK_DEV = 512
REACH = 2
CAP = 2
PICKS = 6
WIDTH = 1536
TILES_DEV = 4
SHARDS = 8
SEQLEN = 4096
NTILES = 32


def mask_tables(key):
    folded = jax.random.fold_in(key, 101)
    key_pool, key_score, key_heavy, key_count = jax.random.split(folded, 4)
    cand_count = TILES_DEV + 2 * REACH * CAP
    offset_list = jnp.array([moved for moved in range(-REACH, REACH + 1) if moved != 0], dtype=jnp.int32)
    shard_ids = jnp.arange(SHARDS, dtype=jnp.int32)
    tile_ids = jnp.arange(TILES_DEV, dtype=jnp.int32)
    pool_scores = jax.random.randint(key_pool, (SHARDS, 2 * REACH, TILES_DEV), 0, 1 << 16, dtype=jnp.int32) * TILES_DEV + tile_ids
    pool_local = lax.top_k(pool_scores, CAP)[1].astype(jnp.int32)
    owner_ids = shard_ids[:, None, None] + offset_list[None, :, None]
    pool_tiles = owner_ids * TILES_DEV + pool_local
    pool_valid = jnp.broadcast_to((owner_ids >= 0) & (owner_ids < SHARDS), pool_local.shape)
    local_tiles = shard_ids[:, None] * TILES_DEV + tile_ids[None, :]
    candidates = jnp.concatenate([local_tiles, pool_tiles.reshape(SHARDS, 2 * REACH * CAP)], axis=1)
    cand_valid = jnp.concatenate([jnp.ones((SHARDS, TILES_DEV), dtype=bool), pool_valid.reshape(SHARDS, 2 * REACH * CAP)], axis=1)
    cand_index = jnp.arange(cand_count, dtype=jnp.int32)
    noise_scores = jax.random.randint(key_score, (SHARDS, TILES_DEV, cand_count), 0, 1 << 16, dtype=jnp.int32) * cand_count + cand_index
    self_slot = cand_index[None, :] == tile_ids[:, None]
    block_index = (cand_index - TILES_DEV) // CAP
    row_of_block = (shard_ids[:, None] + block_index[None, :]) % TILES_DEV
    in_forced = (cand_index >= TILES_DEV)[None, None, :] & (tile_ids[None, :, None] == row_of_block[:, None, :])
    total_score = noise_scores + jnp.where(self_slot[None, :, :], 1 << 26, 0) + jnp.where(in_forced, 1 << 24, 0) - jnp.where(cand_valid[:, None, :], 0, 1 << 27)
    best_index = lax.top_k(total_score, PICKS)[1].astype(jnp.int32)
    spread = jnp.broadcast_to(candidates[:, None, :], (SHARDS, TILES_DEV, cand_count))
    select = jnp.take_along_axis(spread, best_index, axis=2).reshape(NTILES, PICKS).astype(jnp.int32)
    heavy_shard = jax.random.randint(key_heavy, (SHARDS,), 0, 4, dtype=jnp.int32) == 0
    many_picks = jax.random.randint(key_count, (SHARDS, TILES_DEV), PICKS - 2, PICKS + 1, dtype=jnp.int32)
    few_picks = jax.random.randint(jax.random.fold_in(key_count, 3), (SHARDS, TILES_DEV), 2, 4, dtype=jnp.int32)
    counts = jnp.where(heavy_shard[:, None], many_picks, few_picks)
    forced_row = (tile_ids[None, :] - shard_ids[:, None]) % TILES_DEV < 2 * REACH
    counts = jnp.where(forced_row, jnp.maximum(counts, CAP + 1), counts).reshape(NTILES).astype(jnp.int32)
    return (select, counts)


def draw_select(key, part):
    return mask_tables(key)[0]


def draw_counts(key, part):
    return mask_tables(key)[1]


def query_key_tables(key):
    folded = jax.random.fold_in(key, 202)
    key_query, key_key = jax.random.split(folded, 2)
    queries = jax.random.normal(key_query, (2 * SEQLEN, HEADS, HEAD_DIM), jnp.float32)
    keyset = jnp.clip(jax.random.normal(key_key, (2 * SEQLEN, HEADS, HEAD_DIM), jnp.float32), -6.0, 6.0)
    queries = jnp.clip(queries, -200.0, 200.0)
    return (queries.reshape(2 * SEQLEN, HEADS * HEAD_DIM), keyset.reshape(2 * SEQLEN, HEADS * HEAD_DIM))


def draw_query_rows(key, part):
    return query_key_tables(key)[0].astype(jnp.bfloat16)


def draw_key_rows(key, part):
    return query_key_tables(key)[1].astype(jnp.bfloat16)


def shard_levels(own_key, dims, cuts, low, largest):
    def one(dim, shards_of):
        draws = jax.random.uniform(jax.random.fold_in(jax.random.fold_in(own_key, 6), dim), (shards_of,), jnp.float32, low / len(cuts), largest / len(cuts))
        return jnp.repeat(jnp.exp(draws), dims[dim] // shards_of).reshape((-1,) + (1,) * (len(dims) - dim - 1))

    factor_of = one(*cuts[0])
    for cut in cuts[1:]:
        factor_of = factor_of * one(*cut)
    return factor_of


def scatter_about(own_key, dims, deviation, most, shards=(), kind=jnp.bfloat16):
    drawn = deviation * jax.random.normal(own_key, dims, jnp.float32)
    if shards:
        drawn = drawn * shard_levels(own_key, dims, shards, -0.22, 0.18)
    return jnp.clip(drawn, -most, most).astype(kind)


def setup_inputs(seed: int = 0, part: int = 0) -> dict:
    splits = jax.random.split(jax.random.key(seed), 7)
    own_keys = jax.random.split(jax.random.fold_in(splits[6], part), 7)
    query_rows = draw_query_rows(jax.random.fold_in(jax.random.fold_in(splits[6], part), 71), part)
    key_rows = draw_key_rows(jax.random.fold_in(jax.random.fold_in(splits[6], part), 71), part)
    value_rows = scatter_about(own_keys[2], (2 * SEQLEN, WIDTH), 1.0, 6.0, ((0, 16),))
    select = draw_select(jax.random.fold_in(jax.random.fold_in(splits[6], part), 71), part)
    counts = draw_counts(jax.random.fold_in(jax.random.fold_in(splits[6], part), 71), part)
    guide_scale = jnp.clip(jax.random.uniform(own_keys[5], (1,), jnp.float32, 4.0, 8.0), 4.0, 8.0)
    return {"query_rows": query_rows, "key_rows": key_rows, "value_rows": value_rows, "select": select, "counts": counts, "guide_scale": guide_scale}


def attend_tile(query_tile, key_sel, value_sel, alive_slots):
    score_scale = HEAD_DIM ** -0.5
    scores = jnp.einsum("thd,pshd->htps", query_tile.astype(jnp.float32), key_sel.astype(jnp.float32)) * score_scale
    scores = jnp.where(alive_slots[None, None, :, None], scores, -jnp.inf)
    row_max = jnp.max(scores, axis=(2, 3), keepdims=True)
    weights = jnp.exp(scores - row_max)
    denominator = jnp.sum(weights, axis=(2, 3))
    rounded = lax.optimization_barrier(weights.astype(jnp.bfloat16)).astype(jnp.float32)
    weighted = jnp.einsum("htps,pshd->thd", rounded, value_sel.astype(jnp.float32))
    return (weighted / jnp.transpose(denominator)[:, :, None]).astype(jnp.bfloat16)


def branch_major(rows, ntiles):
    split = rows.reshape(SHARDS, 2, TOK_DEV, HEADS * HEAD_DIM)
    return jnp.transpose(split, (1, 0, 2, 3)).reshape(2, ntiles, TILE, HEADS, HEAD_DIM)


def reference(query_rows, key_rows, value_rows, select, counts, guide_scale):
    ntiles = select.shape[0]
    query_tiles = branch_major(query_rows, ntiles)
    key_tiles = branch_major(key_rows, ntiles)
    value_tiles = branch_major(value_rows, ntiles)
    alive_all = jnp.arange(PICKS, dtype=jnp.int32)[None, :] < counts[:, None]
    guidance = guide_scale[0]

    def one_tile(inputs):
        cond_query, uncond_query, chosen, alive_slots = inputs
        cond_out = attend_tile(cond_query, key_tiles[0][chosen], value_tiles[0][chosen], alive_slots)
        uncond = attend_tile(uncond_query, key_tiles[1][chosen], value_tiles[1][chosen], alive_slots)
        cond_wide = lax.optimization_barrier(cond_out).astype(jnp.float32)
        uncond_wide = lax.optimization_barrier(uncond).astype(jnp.float32)
        mixed_out = uncond_wide + guidance * (cond_wide - uncond_wide)
        return mixed_out.astype(jnp.bfloat16).reshape(TILE, HEADS * HEAD_DIM)

    guided = lax.map(one_tile, (query_tiles[0], query_tiles[1], select, alive_all), batch_size=4)
    return guided.reshape(ntiles * TILE, HEADS * HEAD_DIM)
```

```python
import functools
import math

import jax
import jax.numpy as jnp
from jax import lax
from jax.experimental import pallas as pl
from jax.experimental.pallas import tpu as pltpu
from jax.sharding import PartitionSpec as P

HEAD_DIM = 128
TILE = 128
REACH = 2
CAP = 2
FLOWS = 4
PAIR, DIAG, UP, DOWN = range(FLOWS)
AHEAD = 2
GROUP_SHARES = (2, 2, 2, 2, 2, 1, 1)

SMEM = pltpu.SMEM
MESH = pl.DeviceIdType.MESH


def bent_groups(groups, share, planes):
    sizes = [count for _, count in groups[:-1]]
    if not sizes:
        return set()
    rate = share / planes * (sum(sizes) + groups[-1][1]) / sum(sizes)
    chosen, owed = set(), 0.0
    for g, size in enumerate(sizes):
        owed += rate * size
        if owed >= size / 2:
            chosen.add(g)
            owed -= size
    return chosen


def main_kernel(
    ladder,
    groups,
    select_ref,
    counts_ref,
    guide_ref,
    query_hbm,
    key_hbm,
    value_hbm,
    out_ref,
    *refs,
):
    count = len(groups)
    stock, pools, outgoing, relay = (refs[i * count : (i + 1) * count] for i in range(4))
    query_ref, own, away, theirs, send_ref, slots_ref, bias_ref, *sems = refs[4 * count :]
    load_sem, query_sem, send_sem, recv_sem, relay_send, relay_recv, swap_send, swap_recv = sems
    picks = select_ref.shape[0]
    tiles_dev = key_hbm.shape[0]
    half_tiles = tiles_dev // 2
    index = lax.axis_index("seq")
    shard, half = index // 2, index % 2
    shards = lax.axis_size("seq") // 2
    planes = shards // 2
    other = index + 1 - 2 * half
    side = 2 * (shard % 2) - 1
    goes = (-side, side, 2, -2)
    comes = (-side, side, -2, 2)

    def inside(place):
        return (place >= 0) & (place < shards)

    def relayed(sender, g):
        odd = sender % 2
        plane = sender // 2
        share = jnp.where(odd == 1, planes - 1 - plane, plane)
        step = 2 * odd - 1
        bent = jnp.bool_(False)
        for part in range(1, planes if ladder else 0):
            if g in bent_groups(groups, part, planes):
                bent = bent | (share == part)
        return bent & inside(sender) & inside(sender + step) & inside(sender - step)

    barrier = pltpu.get_barrier_semaphore()
    pl.semaphore_signal(barrier, inc=1, device_id={"seq": other}, device_id_type=MESH)
    greeted = jnp.int32(1)
    for offset in goes:
        greeted = greeted + jnp.where(inside(shard + offset), 1, 0)

        @pl.when(inside(shard + offset))
        def _(offset=offset):
            pl.semaphore_signal(
                barrier, inc=1, device_id={"seq": index + 2 * offset}, device_id_type=MESH
            )

    def columns(g):
        first, size = groups[g]
        return pl.ds(first * HEAD_DIM, size * HEAD_DIM)

    def load(g, part, target):
        source = (key_hbm, value_hbm)[part]
        into = (stock[g], pools[g].at[pl.ds(0, tiles_dev)])[target]
        return pltpu.make_async_copy(
            source.at[:, :, columns(g)], into.at[:, part], load_sem.at[g, part, target]
        )

    def load_query():
        return pltpu.make_async_copy(query_hbm, query_ref, query_sem)

    for target in range(2):
        for g in range(count):
            load(g, 0, target).start()
            load(g, 1, target).start()
        if target == 0:
            load_query().start()

    def entries(query_shard):
        first = jnp.clip(query_shard, 0, shards - 1) * tiles_dev
        found = []
        for row in range(tiles_dev):
            count = counts_ref[first + row]
            for pick in range(picks):
                found.append((select_ref[pick, first + row], pick < count))
        return found

    def span(found, owner):
        low, high = jnp.int32(tiles_dev), jnp.int32(-1)
        for tile, live in found:
            local = tile - owner * tiles_dev
            usable = (local >= 0) & (local < tiles_dev) & live
            low = jnp.where(usable, jnp.minimum(low, local), low)
            high = jnp.where(usable, jnp.maximum(high, local), high)
        return jnp.where(high < 0, 0, low), jnp.maximum(high, 0)

    for k in range(FLOWS):
        low, high = span(entries(shard + goes[k]), shard)
        send_ref[CAP * k] = low
        send_ref[CAP * k + 1] = high

    def remote(source, target, sent, landed, device):
        return pltpu.make_async_remote_copy(
            src_ref=source,
            dst_ref=target,
            send_sem=sent,
            recv_sem=landed,
            device_id={"seq": device},
            device_id_type=MESH,
        )

    def landing(g, k):
        return pools[g].at[pl.ds(tiles_dev + CAP * k, CAP)]

    def direct(g, k):
        return remote(
            outgoing[g].at[k], landing(g, k), send_sem.at[g, k], recv_sem.at[g, k], index + 2 * goes[k]
        )

    def first_leg(g):
        return remote(
            outgoing[g].at[DIAG], relay[g], send_sem.at[g, DIAG], relay_recv.at[g], index - 2 * side
        )

    def second_leg(g):
        return remote(
            relay[g], landing(g, DIAG), relay_send.at[g], recv_sem.at[g, DIAG], index - 4 * side
        )

    def swap(g):
        return remote(
            away.at[:, columns(g)], theirs.at[:, columns(g)], swap_send.at[g], swap_recv.at[g], other
        )

    def gather(g):
        load(g, 0, 0).wait()
        load(g, 1, 0).wait()
        for k in range(FLOWS):
            for slot in range(CAP):
                outgoing[g][k, slot] = stock[g][send_ref[CAP * k + slot]]

    def launch(g):
        bent = relayed(shard, g)

        @pl.when(bent)
        def _():
            first_leg(g).start()

        @pl.when(inside(shard + side) & jnp.logical_not(bent))
        def _():
            direct(g, DIAG).start()

        for k in (PAIR, UP, DOWN):

            @pl.when(inside(shard + goes[k]))
            def _(k=k):
                direct(g, k).start()

    def forward(g):
        @pl.when(relayed(shard - side, g))
        def _():
            first_leg(g).wait_recv()
            second_leg(g).start()

    def arrive(g):
        load(g, 0, 1).wait()
        load(g, 1, 1).wait()
        for k in range(FLOWS):

            @pl.when(inside(shard + comes[k]))
            def _(k=k):
                direct(g, k).wait_recv()

    ahead = min(AHEAD, count)
    gather(0)
    pl.semaphore_wait(barrier, greeted)
    for g in range(1, ahead + 1):
        if g < count:
            gather(g)
        launch(g - 1)

    mine = entries(shard)
    lows = [span(mine, shard + comes[k])[0] for k in range(FLOWS)]
    for spot, (tile, live) in enumerate(mine):
        local = tile - shard * tiles_dev
        slot = jnp.where((local >= 0) & (local < tiles_dev), local, 0)
        for k in range(FLOWS):
            there = local - comes[k] * tiles_dev
            second = jnp.where(there == lows[k], 0, 1)
            slot = jnp.where(
                (there >= 0) & (there < tiles_dev), tiles_dev + CAP * k + second, slot
            )
        slots_ref[spot] = slot
        bias_ref[spot] = jnp.where(live, 0.0, -jnp.inf)

    load_query().wait()
    factor = HEAD_DIM**-0.5 * math.log2(math.e)

    def attend(g, mine):
        first, size = groups[g]
        pool = pools[g]
        which = half if mine else 1 - half
        target = own if mine else away

        @pl.loop(0, size)
        def _(h):
            local = pl.ds(pl.multiple_of(h * HEAD_DIM, HEAD_DIM), HEAD_DIM)
            cols = pl.ds(pl.multiple_of((first + h) * HEAD_DIM, HEAD_DIM), HEAD_DIM)
            for step in range(half_tiles):
                tile = which * half_tiles + step
                query = query_ref[pl.ds(pl.multiple_of(tile * TILE, TILE), TILE), cols]
                slots = [slots_ref[tile * picks + p] for p in range(picks)]
                keys = jnp.concatenate([pool[s, 0, :, local] for s in slots], axis=0)
                values = jnp.concatenate([pool[s, 1, :, local] for s in slots], axis=0)
                scores = lax.dot_general(
                    query, keys, (((1,), (1,)), ((), ())), preferred_element_type=jnp.float32
                )
                parts = [
                    scores[:, p * TILE : (p + 1) * TILE] + bias_ref[tile * picks + p]
                    for p in range(picks)
                ]
                top = jnp.max(functools.reduce(jnp.maximum, parts), axis=1, keepdims=True)
                weights = [jnp.exp2((part - top) * factor) for part in parts]
                total = jnp.sum(functools.reduce(jnp.add, weights), axis=1, keepdims=True)
                rounded = jnp.concatenate([w.astype(jnp.bfloat16) for w in weights], axis=1)
                mixed = jnp.dot(rounded, values, preferred_element_type=jnp.float32)
                target[step * TILE : (step + 1) * TILE, cols] = (mixed / total).astype(jnp.bfloat16)

    def combine(g):
        swap(g).wait_recv()
        from_me = own[:, columns(g)].astype(jnp.float32)
        from_other = theirs[:, columns(g)].astype(jnp.float32)
        cond = jnp.where(half == 0, from_me, from_other)
        uncond = jnp.where(half == 0, from_other, from_me)
        out_ref[:, columns(g)] = (uncond + guide_ref[0] * (cond - uncond)).astype(jnp.bfloat16)

    for g in range(count):
        forward(g)
        if g + ahead + 1 < count:
            gather(g + ahead + 1)
        if g + ahead < count:
            launch(g + ahead)
        arrive(g)
        attend(g, False)
        swap(g).start()
        attend(g, True)
        if g > 0:
            combine(g - 1)
    combine(count - 1)

    for g in range(count):
        bent = relayed(shard, g)

        @pl.when(bent)
        def _(g=g):
            first_leg(g).wait_send()

        @pl.when(inside(shard + side) & jnp.logical_not(bent))
        def _(g=g):
            direct(g, DIAG).wait_send()

        for k in (PAIR, UP, DOWN):

            @pl.when(inside(shard + goes[k]))
            def _(g=g, k=k):
                direct(g, k).wait_send()

        @pl.when(relayed(shard - side, g))
        def _(g=g):
            second_leg(g).wait_send()

        swap(g).wait_send()


def head_groups(heads):
    shares = GROUP_SHARES if heads == sum(GROUP_SHARES) else (1,) * heads
    groups, first = [], 0
    for share in shares:
        groups.append((first, share))
        first += share
    return groups


def body(ladder, query_rows, key_rows, value_rows, select, counts, guide_scale):
    tokens, width = query_rows.shape
    heads = width // HEAD_DIM
    tiles_dev = tokens // TILE
    picks = select.shape[1]
    half_rows = tokens // 2
    rows = jnp.bfloat16
    dma = pltpu.SemaphoreType.DMA
    smem = pl.BlockSpec(memory_space=SMEM)
    hbm = pl.BlockSpec(memory_space=pl.ANY)
    groups = head_groups(heads)
    count = len(groups)
    half = pltpu.VMEM((half_rows, width), rows)

    def scratch(*lead):
        return [pltpu.VMEM((*lead, 2, TILE, size * HEAD_DIM), rows) for _, size in groups]

    return pl.pallas_call(
        functools.partial(main_kernel, ladder, groups),
        out_shape=jax.ShapeDtypeStruct((half_rows, width), rows),
        in_specs=[smem] * 3 + [hbm] * 3,
        out_specs=pl.BlockSpec(memory_space=pltpu.VMEM),
        scratch_shapes=[
            *scratch(tiles_dev),
            *scratch(tiles_dev + CAP * FLOWS),
            *scratch(FLOWS, CAP),
            *scratch(CAP),
            pltpu.VMEM((tokens, width), rows),
            half,
            half,
            half,
            SMEM((CAP * FLOWS,), jnp.int32),
            SMEM((tiles_dev * picks,), jnp.int32),
            SMEM((tiles_dev * picks,), jnp.float32),
            dma((count, 2, 2)),
            dma(()),
            dma((count, FLOWS)),
            dma((count, FLOWS)),
            dma((count,)),
            dma((count,)),
            dma((count,)),
            dma((count,)),
        ],
        compiler_params=pltpu.CompilerParams(
            collective_id=0, has_side_effects=True, vmem_limit_bytes=60000 * 1024
        ),
        name="main",
    )(
        select.T,
        counts,
        guide_scale,
        query_rows,
        key_rows.reshape(tiles_dev, TILE, width),
        value_rows.reshape(tiles_dev, TILE, width),
    )


def is_ladder(mesh):
    devices = mesh.devices.reshape(mesh.shape["groups"], -1)[0][::2]
    places = [getattr(device, "coords", None) for device in devices]
    if any(place is None for place in places) or len(places) % 2:
        return False

    def hops(a, b):
        return sum(abs(p - q) for p, q in zip(places[a], places[b], strict=True))

    rungs = all(hops(s, s + 1) == 1 for s in range(0, len(places), 2))
    return rungs and all(hops(s, s + 2) == 1 for s in range(len(places) - 2))


def solution(mesh):
    in_specs = (
        P(("groups", "seq"), None),
        P(("groups", "seq"), None),
        P(("groups", "seq"), None),
        P("groups", None),
        P("groups"),
        P("groups"),
    )
    out_specs = P(("groups", "seq"), None)
    return jax.shard_map(
        functools.partial(body, is_ladder(mesh)),
        mesh=mesh,
        in_specs=in_specs,
        out_specs=out_specs,
        check_vma=False,
    )
```

```python
import functools
import math

import jax
import jax.numpy as jnp
from jax import lax
from jax.experimental import pallas as pl
from jax.experimental.pallas import tpu as pltpu
from jax.sharding import PartitionSpec as P

HEAD_DIM = 128
TILE = 128
REACH = 2
CAP = 2
FLOWS = 4
PAIR, DIAG, UP, DOWN = range(FLOWS)
AHEAD = 2
GROUP_SHARES = (2, 2, 2, 2, 2, 1, 1)

SMEM = pltpu.SMEM
MESH = pl.DeviceIdType.MESH


def near_groups(groups, share, planes):
    chosen, owed = set(), 0.0
    for g, (_, size) in enumerate(groups):
        owed += share / planes * size
        if owed >= size / 2:
            chosen.add(g)
            owed -= size
    return chosen


def main_kernel(
    ladder,
    groups,
    select_ref,
    counts_ref,
    guide_ref,
    query_hbm,
    key_hbm,
    value_hbm,
    out_ref,
    *refs,
):
    count = len(groups)
    stock, pools, outgoing, *relay = (refs[i * count : (i + 1) * count] for i in range(5))
    query_ref, own, away, theirs, send_ref, slots_ref, bias_ref, *sems = refs[5 * count :]
    load_sem, query_sem, send_sem, recv_sem, relay_send, relay_recv, swap_send, swap_recv = sems
    picks = select_ref.shape[0]
    tiles_dev = key_hbm.shape[0]
    half_tiles = tiles_dev // 2
    index = lax.axis_index("seq")
    shard, half = index // 2, index % 2
    shards = lax.axis_size("seq") // 2
    planes = shards // 2
    other = index + 1 - 2 * half
    side = 2 * (shard % 2) - 1
    goes = (-side, side, 2, -2)
    comes = (-side, side, -2, 2)

    def inside(place):
        return (place >= 0) & (place < shards)

    def takes(sender, g, via):
        plane = sender // 2
        share = jnp.where(sender % 2 == 1, planes - 1 - plane, plane)
        near = jnp.bool_(False)
        for part in range(1, planes):
            if g in near_groups(groups, part, planes):
                near = near | (share == part)
        wanted = inside(sender) & inside(sender + 2 * (sender % 2) - 1)
        return wanted & (near if via == 0 else jnp.logical_not(near))

    barrier = pltpu.get_barrier_semaphore()
    pl.semaphore_signal(barrier, inc=1, device_id={"seq": other}, device_id_type=MESH)
    greeted = jnp.int32(1)
    for offset in goes:
        greeted = greeted + jnp.where(inside(shard + offset), 1, 0)

        @pl.when(inside(shard + offset))
        def _(offset=offset):
            pl.semaphore_signal(
                barrier, inc=1, device_id={"seq": index + 2 * offset}, device_id_type=MESH
            )

    def columns(g):
        first, size = groups[g]
        return pl.ds(first * HEAD_DIM, size * HEAD_DIM)

    def load(g, part, target):
        source = (key_hbm, value_hbm)[part]
        into = (stock[g], pools[g].at[pl.ds(0, tiles_dev)])[target]
        return pltpu.make_async_copy(
            source.at[:, :, columns(g)], into.at[:, part], load_sem.at[g, part, target]
        )

    def load_query():
        return pltpu.make_async_copy(query_hbm, query_ref, query_sem)

    for target in range(2):
        for g in range(count):
            load(g, 0, target).start()
            load(g, 1, target).start()
        if target == 0:
            load_query().start()

    def entries(query_shard):
        first = jnp.clip(query_shard, 0, shards - 1) * tiles_dev
        found = []
        for row in range(tiles_dev):
            count = counts_ref[first + row]
            for pick in range(picks):
                found.append((select_ref[pick, first + row], pick < count))
        return found

    def span(found, owner):
        low, high = jnp.int32(tiles_dev), jnp.int32(-1)
        for tile, live in found:
            local = tile - owner * tiles_dev
            usable = (local >= 0) & (local < tiles_dev) & live
            low = jnp.where(usable, jnp.minimum(low, local), low)
            high = jnp.where(usable, jnp.maximum(high, local), high)
        return jnp.where(high < 0, 0, low), jnp.maximum(high, 0)

    for k in range(FLOWS):
        low, high = span(entries(shard + goes[k]), shard)
        send_ref[CAP * k] = low
        send_ref[CAP * k + 1] = high

    def remote(source, target, sent, landed, device):
        return pltpu.make_async_remote_copy(
            src_ref=source,
            dst_ref=target,
            send_sem=sent,
            recv_sem=landed,
            device_id={"seq": device},
            device_id_type=MESH,
        )

    def landing(g, k):
        return pools[g].at[pl.ds(tiles_dev + CAP * k, CAP)]

    def direct(g, k):
        return remote(
            outgoing[g].at[k], landing(g, k), send_sem.at[g, k], recv_sem.at[g, k], index + 2 * goes[k]
        )

    def first_leg(g, via):
        return remote(
            outgoing[g].at[DIAG],
            relay[via][g],
            send_sem.at[g, DIAG],
            relay_recv.at[g, via],
            index + 2 * (-side, 2 * side)[via],
        )

    def second_leg(g, via):
        return remote(
            relay[via][g],
            landing(g, DIAG),
            relay_send.at[g, via],
            recv_sem.at[g, DIAG],
            index - 2 * (2 * side, side)[via],
        )

    def swap(g):
        return remote(
            away.at[:, columns(g)], theirs.at[:, columns(g)], swap_send.at[g], swap_recv.at[g], other
        )

    def gather(g):
        load(g, 0, 0).wait()
        load(g, 1, 0).wait()
        for k in range(FLOWS):
            for slot in range(CAP):
                outgoing[g][k, slot] = stock[g][send_ref[CAP * k + slot]]

    def diagonal(g, act):
        if ladder:
            for via in range(2):

                @pl.when(takes(shard, g, via))
                def _(via=via):
                    act(first_leg(g, via))

        else:

            @pl.when(inside(shard + side))
            def _():
                act(direct(g, DIAG))

    def launch(g):
        if g + 1 < count:
            diagonal(g + 1, lambda copy: copy.start())
        for k in (PAIR, UP, DOWN):

            @pl.when(inside(shard + goes[k]))
            def _(k=k):
                direct(g, k).start()

    def forward(g):
        for via in range(2 if ladder and g < count else 0):

            @pl.when(takes(shard - (side, 2 * side)[via], g, via))
            def _(via=via):
                first_leg(g, via).wait_recv()
                second_leg(g, via).start()

    def arrive(g):
        load(g, 0, 1).wait()
        load(g, 1, 1).wait()
        for k in range(FLOWS):

            @pl.when(inside(shard + comes[k]))
            def _(k=k):
                direct(g, k).wait_recv()

    ahead = min(AHEAD, count)
    gather(0)
    pl.semaphore_wait(barrier, greeted)
    diagonal(0, lambda copy: copy.start())
    for g in range(min(ahead + 1, count)):
        if g + 1 < count:
            gather(g + 1)
        if g < ahead:
            launch(g)

    mine = entries(shard)
    lows = [span(mine, shard + comes[k])[0] for k in range(FLOWS)]
    for spot, (tile, live) in enumerate(mine):
        local = tile - shard * tiles_dev
        slot = jnp.where((local >= 0) & (local < tiles_dev), local, 0)
        for k in range(FLOWS):
            there = local - comes[k] * tiles_dev
            second = jnp.where(there == lows[k], 0, 1)
            slot = jnp.where(
                (there >= 0) & (there < tiles_dev), tiles_dev + CAP * k + second, slot
            )
        slots_ref[spot] = slot
        bias_ref[spot] = jnp.where(live, 0.0, -jnp.inf)

    load_query().wait()
    factor = HEAD_DIM**-0.5 * math.log2(math.e)

    def attend(g, mine):
        first, size = groups[g]
        pool = pools[g]
        which = half if mine else 1 - half
        target = own if mine else away

        @pl.loop(0, size)
        def _(h):
            local = pl.ds(pl.multiple_of(h * HEAD_DIM, HEAD_DIM), HEAD_DIM)
            cols = pl.ds(pl.multiple_of((first + h) * HEAD_DIM, HEAD_DIM), HEAD_DIM)
            for step in range(half_tiles):
                tile = which * half_tiles + step
                query = query_ref[pl.ds(pl.multiple_of(tile * TILE, TILE), TILE), cols]
                slots = [slots_ref[tile * picks + p] for p in range(picks)]
                keys = jnp.concatenate([pool[s, 0, :, local] for s in slots], axis=0)
                values = jnp.concatenate([pool[s, 1, :, local] for s in slots], axis=0)
                scores = lax.dot_general(
                    query, keys, (((1,), (1,)), ((), ())), preferred_element_type=jnp.float32
                )
                parts = [
                    scores[:, p * TILE : (p + 1) * TILE] + bias_ref[tile * picks + p]
                    for p in range(picks)
                ]
                top = jnp.max(functools.reduce(jnp.maximum, parts), axis=1, keepdims=True)
                weights = [jnp.exp2((part - top) * factor) for part in parts]
                total = jnp.sum(functools.reduce(jnp.add, weights), axis=1, keepdims=True)
                rounded = jnp.concatenate([w.astype(jnp.bfloat16) for w in weights], axis=1)
                mixed = jnp.dot(rounded, values, preferred_element_type=jnp.float32)
                target[step * TILE : (step + 1) * TILE, cols] = (mixed / total).astype(jnp.bfloat16)

    def combine(g):
        swap(g).wait_recv()
        from_me = own[:, columns(g)].astype(jnp.float32)
        from_other = theirs[:, columns(g)].astype(jnp.float32)
        cond = jnp.where(half == 0, from_me, from_other)
        uncond = jnp.where(half == 0, from_other, from_me)
        out_ref[:, columns(g)] = (uncond + guide_ref[0] * (cond - uncond)).astype(jnp.bfloat16)

    forward(0)
    for g in range(count):
        forward(g + 1)
        if g + ahead + 2 < count:
            gather(g + ahead + 2)
        if g + ahead < count:
            launch(g + ahead)
        arrive(g)
        attend(g, False)
        swap(g).start()
        attend(g, True)
        if g > 0:
            combine(g - 1)
    combine(count - 1)

    for g in range(count):
        diagonal(g, lambda copy: copy.wait_send())

        for k in (PAIR, UP, DOWN):

            @pl.when(inside(shard + goes[k]))
            def _(g=g, k=k):
                direct(g, k).wait_send()

        for via in range(2 if ladder else 0):

            @pl.when(takes(shard - (side, 2 * side)[via], g, via))
            def _(g=g, via=via):
                second_leg(g, via).wait_send()

        swap(g).wait_send()


def head_groups(heads):
    shares = GROUP_SHARES if heads == sum(GROUP_SHARES) else (1,) * heads
    groups, first = [], 0
    for share in shares:
        groups.append((first, share))
        first += share
    return groups


def body(ladder, query_rows, key_rows, value_rows, select, counts, guide_scale):
    tokens, width = query_rows.shape
    heads = width // HEAD_DIM
    tiles_dev = tokens // TILE
    picks = select.shape[1]
    half_rows = tokens // 2
    rows = jnp.bfloat16
    dma = pltpu.SemaphoreType.DMA
    smem = pl.BlockSpec(memory_space=SMEM)
    hbm = pl.BlockSpec(memory_space=pl.ANY)
    groups = head_groups(heads)
    count = len(groups)
    half = pltpu.VMEM((half_rows, width), rows)

    def scratch(*lead):
        return [pltpu.VMEM((*lead, 2, TILE, size * HEAD_DIM), rows) for _, size in groups]

    return pl.pallas_call(
        functools.partial(main_kernel, ladder, groups),
        out_shape=jax.ShapeDtypeStruct((half_rows, width), rows),
        in_specs=[smem] * 3 + [hbm] * 3,
        out_specs=pl.BlockSpec(memory_space=pltpu.VMEM),
        scratch_shapes=[
            *scratch(tiles_dev),
            *scratch(tiles_dev + CAP * FLOWS),
            *scratch(FLOWS, CAP),
            *scratch(CAP),
            *scratch(CAP),
            pltpu.VMEM((tokens, width), rows),
            half,
            half,
            half,
            SMEM((CAP * FLOWS,), jnp.int32),
            SMEM((tiles_dev * picks,), jnp.int32),
            SMEM((tiles_dev * picks,), jnp.float32),
            dma((count, 2, 2)),
            dma(()),
            dma((count, FLOWS)),
            dma((count, FLOWS)),
            dma((count, 2)),
            dma((count, 2)),
            dma((count,)),
            dma((count,)),
        ],
        compiler_params=pltpu.CompilerParams(
            collective_id=0, has_side_effects=True, vmem_limit_bytes=60000 * 1024
        ),
        name="main",
    )(
        select.T,
        counts,
        guide_scale,
        query_rows,
        key_rows.reshape(tiles_dev, TILE, width),
        value_rows.reshape(tiles_dev, TILE, width),
    )


def is_ladder(mesh):
    devices = mesh.devices.reshape(mesh.shape["groups"], -1)[0][::2]
    places = [getattr(device, "coords", None) for device in devices]
    if any(place is None for place in places) or len(places) % 2:
        return False

    def hops(a, b):
        return sum(abs(p - q) for p, q in zip(places[a], places[b], strict=True))

    rungs = all(hops(s, s + 1) == 1 for s in range(0, len(places), 2))
    return rungs and all(hops(s, s + 2) == 1 for s in range(len(places) - 2))


def solution(mesh):
    in_specs = (
        P(("groups", "seq"), None),
        P(("groups", "seq"), None),
        P(("groups", "seq"), None),
        P("groups", None),
        P("groups"),
        P("groups"),
    )
    out_specs = P(("groups", "seq"), None)
    return jax.shard_map(
        functools.partial(body, is_ladder(mesh)),
        mesh=mesh,
        in_specs=in_specs,
        out_specs=out_specs,
        check_vma=False,
    )
```

```python
import functools
import math

import jax
import jax.numpy as jnp
from jax import lax
from jax.experimental import pallas as pl
from jax.experimental.pallas import tpu as pltpu
from jax.sharding import PartitionSpec as P

HEAD_DIM = 128
TILE = 128
REACH = 2
CAP = 2
FLOWS = 4
PAIR, DIAG, UP, DOWN = range(FLOWS)
AHEAD = 2
GROUP_SHARES = (2, 2, 2, 2, 2, 1, 1)

SMEM = pltpu.SMEM
MESH = pl.DeviceIdType.MESH


def near_groups(groups, share, planes):
    chosen, owed = set(), 0.0
    for g, (_, size) in enumerate(groups):
        owed += share / planes * size
        if owed >= size / 2:
            chosen.add(g)
            owed -= size
    return chosen


def main_kernel(
    ladder,
    groups,
    select_hbm,
    counts_hbm,
    guide_ref,
    query_hbm,
    key_hbm,
    value_hbm,
    out_ref,
    *refs,
):
    count = len(groups)
    stock, pools, outgoing, *relay = (refs[i * count : (i + 1) * count] for i in range(5))
    select_ref, counts_ref, query_ref, own, away, theirs, send_ref, slots_ref, bias_ref, *sems = refs[5 * count :]
    load_sem, query_sem, send_sem, recv_sem, relay_send, relay_recv, swap_send, swap_recv, table_sem = sems
    picks = select_hbm.shape[0]
    tiles_dev = key_hbm.shape[0]
    half_tiles = tiles_dev // 2
    index = lax.axis_index("seq")
    shard, half = index // 2, index % 2
    shards = lax.axis_size("seq") // 2
    planes = shards // 2
    other = index + 1 - 2 * half
    side = 2 * (shard % 2) - 1
    goes = (-side, side, 2, -2)
    comes = (-side, side, -2, 2)

    def inside(place):
        return (place >= 0) & (place < shards)

    def takes(sender, g, via):
        plane = sender // 2
        share = jnp.where(sender % 2 == 1, planes - 1 - plane, plane)
        near = jnp.bool_(False)
        for part in range(1, planes):
            if g in near_groups(groups, part, planes):
                near = near | (share == part)
        wanted = inside(sender) & inside(sender + 2 * (sender % 2) - 1)
        return wanted & (near if via == 0 else jnp.logical_not(near))

    barrier = pltpu.get_barrier_semaphore()
    pl.semaphore_signal(barrier, inc=1, device_id={"seq": other}, device_id_type=MESH)
    greeted = jnp.int32(1)
    for offset in goes:
        greeted = greeted + jnp.where(inside(shard + offset), 1, 0)

        @pl.when(inside(shard + offset))
        def _(offset=offset):
            pl.semaphore_signal(
                barrier, inc=1, device_id={"seq": index + 2 * offset}, device_id_type=MESH
            )

    tables = [
        pltpu.make_async_copy(source, target, table_sem.at[i])
        for i, (source, target) in enumerate(((select_hbm, select_ref), (counts_hbm, counts_ref)))
    ]
    for copy in tables:
        copy.start()

    def columns(g):
        first, size = groups[g]
        return pl.ds(first * HEAD_DIM, size * HEAD_DIM)

    def load(g, part, target):
        source = (key_hbm, value_hbm)[part]
        into = (stock[g], pools[g].at[pl.ds(0, tiles_dev)])[target]
        return pltpu.make_async_copy(
            source.at[:, :, columns(g)], into.at[:, part], load_sem.at[g, part, target]
        )

    def load_query():
        return pltpu.make_async_copy(query_hbm, query_ref, query_sem)

    for target in range(2):
        for g in range(count):
            load(g, 0, target).start()
            load(g, 1, target).start()
        if target == 0:
            load_query().start()

    for copy in tables:
        copy.wait()

    def entries(query_shard):
        first = jnp.clip(query_shard, 0, shards - 1) * tiles_dev
        found = []
        for row in range(tiles_dev):
            count = counts_ref[first + row]
            for pick in range(picks):
                found.append((select_ref[pick, first + row], pick < count))
        return found

    def span(found, owner):
        low, high = jnp.int32(tiles_dev), jnp.int32(-1)
        for tile, live in found:
            local = tile - owner * tiles_dev
            usable = (local >= 0) & (local < tiles_dev) & live
            low = jnp.where(usable, jnp.minimum(low, local), low)
            high = jnp.where(usable, jnp.maximum(high, local), high)
        return jnp.where(high < 0, 0, low), jnp.maximum(high, 0)

    for k in range(FLOWS):
        low, high = span(entries(shard + goes[k]), shard)
        send_ref[CAP * k] = low
        send_ref[CAP * k + 1] = high

    def remote(source, target, sent, landed, device):
        return pltpu.make_async_remote_copy(
            src_ref=source,
            dst_ref=target,
            send_sem=sent,
            recv_sem=landed,
            device_id={"seq": device},
            device_id_type=MESH,
        )

    def landing(g, k):
        return pools[g].at[pl.ds(tiles_dev + CAP * k, CAP)]

    def direct(g, k):
        return remote(
            outgoing[g].at[k], landing(g, k), send_sem.at[g, k], recv_sem.at[g, k], index + 2 * goes[k]
        )

    def first_leg(g, via):
        return remote(
            outgoing[g].at[DIAG],
            relay[via][g],
            send_sem.at[g, DIAG],
            relay_recv.at[g, via],
            index + 2 * (-side, 2 * side)[via],
        )

    def second_leg(g, via):
        return remote(
            relay[via][g],
            landing(g, DIAG),
            relay_send.at[g, via],
            recv_sem.at[g, DIAG],
            index - 2 * (2 * side, side)[via],
        )

    def swap(g):
        return remote(
            away.at[:, columns(g)], theirs.at[:, columns(g)], swap_send.at[g], swap_recv.at[g], other
        )

    def gather(g):
        load(g, 0, 0).wait()
        load(g, 1, 0).wait()
        for k in range(FLOWS):
            for slot in range(CAP):
                outgoing[g][k, slot] = stock[g][send_ref[CAP * k + slot]]

    def diagonal(g, act):
        if ladder:
            for via in range(2):

                @pl.when(takes(shard, g, via))
                def _(via=via):
                    act(first_leg(g, via))

        else:

            @pl.when(inside(shard + side))
            def _():
                act(direct(g, DIAG))

    def launch(g):
        if g + 1 < count:
            diagonal(g + 1, lambda copy: copy.start())
        for k in (PAIR, UP, DOWN):

            @pl.when(inside(shard + goes[k]))
            def _(k=k):
                direct(g, k).start()

    def forward(g):
        for via in range(2 if ladder and g < count else 0):

            @pl.when(takes(shard - (side, 2 * side)[via], g, via))
            def _(via=via):
                first_leg(g, via).wait_recv()
                second_leg(g, via).start()

    def arrive(g):
        load(g, 0, 1).wait()
        load(g, 1, 1).wait()
        for k in range(FLOWS):

            @pl.when(inside(shard + comes[k]))
            def _(k=k):
                direct(g, k).wait_recv()

    ahead = min(AHEAD, count)
    gather(0)
    pl.semaphore_wait(barrier, greeted)
    diagonal(0, lambda copy: copy.start())
    for g in range(min(ahead + 1, count)):
        if g + 1 < count:
            gather(g + 1)
        if g < ahead:
            launch(g)

    mine = entries(shard)
    lows = [span(mine, shard + comes[k])[0] for k in range(FLOWS)]
    for spot, (tile, live) in enumerate(mine):
        local = tile - shard * tiles_dev
        slot = jnp.where((local >= 0) & (local < tiles_dev), local, 0)
        for k in range(FLOWS):
            there = local - comes[k] * tiles_dev
            second = jnp.where(there == lows[k], 0, 1)
            slot = jnp.where(
                (there >= 0) & (there < tiles_dev), tiles_dev + CAP * k + second, slot
            )
        slots_ref[spot] = slot
        bias_ref[spot] = jnp.where(live, 0.0, -jnp.inf)

    load_query().wait()
    factor = HEAD_DIM**-0.5 * math.log2(math.e)

    def attend(g, mine):
        first, size = groups[g]
        pool = pools[g]
        which = half if mine else 1 - half
        target = own if mine else away

        @pl.loop(0, size)
        def _(h):
            local = pl.ds(pl.multiple_of(h * HEAD_DIM, HEAD_DIM), HEAD_DIM)
            cols = pl.ds(pl.multiple_of((first + h) * HEAD_DIM, HEAD_DIM), HEAD_DIM)
            for step in range(half_tiles):
                tile = which * half_tiles + step
                query = query_ref[pl.ds(pl.multiple_of(tile * TILE, TILE), TILE), cols]
                slots = [slots_ref[tile * picks + p] for p in range(picks)]
                keys = jnp.concatenate([pool[s, 0, :, local] for s in slots], axis=0)
                values = jnp.concatenate([pool[s, 1, :, local] for s in slots], axis=0)
                scores = lax.dot_general(
                    query, keys, (((1,), (1,)), ((), ())), preferred_element_type=jnp.float32
                )
                parts = [
                    scores[:, p * TILE : (p + 1) * TILE] + bias_ref[tile * picks + p]
                    for p in range(picks)
                ]
                top = jnp.max(functools.reduce(jnp.maximum, parts), axis=1, keepdims=True)
                weights = [jnp.exp2((part - top) * factor) for part in parts]
                total = jnp.sum(functools.reduce(jnp.add, weights), axis=1, keepdims=True)
                rounded = jnp.concatenate([w.astype(jnp.bfloat16) for w in weights], axis=1)
                mixed = jnp.dot(rounded, values, preferred_element_type=jnp.float32)
                target[step * TILE : (step + 1) * TILE, cols] = (mixed / total).astype(jnp.bfloat16)

    def combine(g):
        swap(g).wait_recv()
        from_me = own[:, columns(g)].astype(jnp.float32)
        from_other = theirs[:, columns(g)].astype(jnp.float32)
        cond = jnp.where(half == 0, from_me, from_other)
        uncond = jnp.where(half == 0, from_other, from_me)
        out_ref[:, columns(g)] = (uncond + guide_ref[0] * (cond - uncond)).astype(jnp.bfloat16)

    forward(0)
    for g in range(count):
        forward(g + 1)
        if g + ahead + 2 < count:
            gather(g + ahead + 2)
        if g + ahead < count:
            launch(g + ahead)
        arrive(g)
        attend(g, False)
        swap(g).start()
        attend(g, True)
        if g > 0:
            combine(g - 1)
    combine(count - 1)

    for g in range(count):
        diagonal(g, lambda copy: copy.wait_send())

        for k in (PAIR, UP, DOWN):

            @pl.when(inside(shard + goes[k]))
            def _(g=g, k=k):
                direct(g, k).wait_send()

        for via in range(2 if ladder else 0):

            @pl.when(takes(shard - (side, 2 * side)[via], g, via))
            def _(g=g, via=via):
                second_leg(g, via).wait_send()

        swap(g).wait_send()


def head_groups(heads):
    shares = GROUP_SHARES if heads == sum(GROUP_SHARES) else (1,) * heads
    groups, first = [], 0
    for share in shares:
        groups.append((first, share))
        first += share
    return groups


def body(ladder, query_rows, key_rows, value_rows, select, counts, guide_scale):
    tokens, width = query_rows.shape
    heads = width // HEAD_DIM
    tiles_dev = tokens // TILE
    picks = select.shape[1]
    half_rows = tokens // 2
    rows = jnp.bfloat16
    dma = pltpu.SemaphoreType.DMA
    hbm = pl.BlockSpec(memory_space=pl.ANY)
    groups = head_groups(heads)
    count = len(groups)
    half = pltpu.VMEM((half_rows, width), rows)

    def scratch(*lead):
        return [pltpu.VMEM((*lead, 2, TILE, size * HEAD_DIM), rows) for _, size in groups]

    return pl.pallas_call(
        functools.partial(main_kernel, ladder, groups),
        out_shape=pltpu.VMEM((half_rows, width), rows),
        in_specs=[hbm, hbm, pl.BlockSpec(memory_space=SMEM), hbm, hbm, hbm],
        out_specs=pl.BlockSpec(memory_space=pltpu.VMEM),
        scratch_shapes=[
            *scratch(tiles_dev),
            *scratch(tiles_dev + CAP * FLOWS),
            *scratch(FLOWS, CAP),
            *scratch(CAP),
            *scratch(CAP),
            SMEM((picks, select.shape[0]), jnp.int32),
            SMEM(counts.shape, jnp.int32),
            pltpu.VMEM((tokens, width), rows),
            half,
            half,
            half,
            SMEM((CAP * FLOWS,), jnp.int32),
            SMEM((tiles_dev * picks,), jnp.int32),
            SMEM((tiles_dev * picks,), jnp.float32),
            dma((count, 2, 2)),
            dma(()),
            dma((count, FLOWS)),
            dma((count, FLOWS)),
            dma((count, 2)),
            dma((count, 2)),
            dma((count,)),
            dma((count,)),
            dma((2,)),
        ],
        compiler_params=pltpu.CompilerParams(
            collective_id=0, has_side_effects=True, vmem_limit_bytes=60000 * 1024
        ),
        name="main",
    )(
        select.T,
        counts,
        guide_scale,
        query_rows,
        key_rows.reshape(tiles_dev, TILE, width),
        value_rows.reshape(tiles_dev, TILE, width),
    )


def is_ladder(mesh):
    devices = mesh.devices.reshape(mesh.shape["groups"], -1)[0][::2]
    places = [getattr(device, "coords", None) for device in devices]
    if any(place is None for place in places) or len(places) % 2:
        return False

    def hops(a, b):
        return sum(abs(p - q) for p, q in zip(places[a], places[b], strict=True))

    rungs = all(hops(s, s + 1) == 1 for s in range(0, len(places), 2))
    return rungs and all(hops(s, s + 2) == 1 for s in range(len(places) - 2))


def solution(mesh):
    in_specs = (
        P(("groups", "seq"), None),
        P(("groups", "seq"), None),
        P(("groups", "seq"), None),
        P("groups", None),
        P("groups"),
        P("groups"),
    )
    out_specs = P(("groups", "seq"), None)
    return jax.shard_map(
        functools.partial(body, is_ladder(mesh)),
        mesh=mesh,
        in_specs=in_specs,
        out_specs=out_specs,
        check_vma=False,
    )
```

```python
import functools
import math

import jax
import jax.numpy as jnp
from jax import lax
from jax.experimental import pallas as pl
from jax.experimental.pallas import tpu as pltpu
from jax.sharding import PartitionSpec as P

HEAD_DIM = 128
TILE = 128
REACH = 2
CAP = 2
FLOWS = 4
PAIR, DIAG, UP, DOWN = range(FLOWS)
AHEAD = 2
GROUP_SHARES = (2, 2, 2, 2, 2, 1, 1)

SMEM = pltpu.SMEM
MESH = pl.DeviceIdType.MESH


def near_groups(groups, share, planes):
    chosen, owed = set(), 0.0
    for g, (_, size) in enumerate(groups):
        owed += share / planes * size
        if owed >= size / 2:
            chosen.add(g)
            owed -= size
    return chosen


def main_kernel(
    ladder,
    groups,
    select_hbm,
    counts_hbm,
    guide_ref,
    query_hbm,
    key_hbm,
    value_hbm,
    out_ref,
    *refs,
):
    count = len(groups)
    pieces = pieces_of(groups)
    units = unit_numbers(groups)
    refs = list(refs)
    stock, pools, outgoing, *relay = (
        [[refs.pop(0) for _ in pieces[g]] for g in range(count)] for _ in range(5)
    )
    select_ref, counts_ref, query_ref, own, away, theirs, held, *rest = refs
    send_ref, slots_ref, bias_ref, *sems = rest
    stock_sem, pool_sem, query_sem, send_sem, recv_sem, relay_send, relay_recv = sems[:7]
    swap_send, swap_recv, table_sem = sems[7:]
    picks = select_hbm.shape[0]
    tiles_dev = key_hbm.shape[0]
    half_tiles = tiles_dev // 2
    index = lax.axis_index("seq")
    shard, half = index // 2, index % 2
    shards = lax.axis_size("seq") // 2
    planes = shards // 2
    other = index + 1 - 2 * half
    side = 2 * (shard % 2) - 1
    goes = (-side, side, 2, -2)
    comes = (-side, side, -2, 2)

    def inside(place):
        return (place >= 0) & (place < shards)

    def share_of(sender):
        plane = sender // 2
        return jnp.where(sender % 2 == 1, planes - 1 - plane, plane)

    def crosses(sender):
        return inside(sender) & inside(sender + 2 * (sender % 2) - 1)

    def takes(sender, g, via):
        near = jnp.bool_(False)
        for part in range(1, planes):
            if g in near_groups(groups, part, planes):
                near = near | (share_of(sender) == part)
        return crosses(sender) & (near if via == 0 else jnp.logical_not(near))

    barrier = pltpu.get_barrier_semaphore()
    pl.semaphore_signal(barrier, inc=1, device_id={"seq": other}, device_id_type=MESH)
    greeted = jnp.int32(1)
    for offset in (-side, 2, -2) if ladder else goes:
        greeted = greeted + jnp.where(inside(shard + offset), 1, 0)

        @pl.when(inside(shard + offset))
        def _(offset=offset):
            pl.semaphore_signal(
                barrier, inc=1, device_id={"seq": index + 2 * offset}, device_id_type=MESH
            )

    tables = [
        pltpu.make_async_copy(source, target, table_sem.at[i])
        for i, (source, target) in enumerate(((select_hbm, select_ref), (counts_hbm, counts_ref)))
    ]
    for copy in tables:
        copy.start()

    def piece_of(g, part):
        return next(p for p, parts in enumerate(pieces[g]) if part in parts)

    def inner_of(g, part):
        return pieces[g][piece_of(g, part)].index(part)

    def columns(g):
        first, size = groups[g]
        return pl.ds(first * HEAD_DIM, size * HEAD_DIM)

    def load(g, part, target):
        source = (key_hbm, value_hbm)[part]
        into = (stock, pools)[target][g][piece_of(g, part)]
        return pltpu.make_async_copy(
            source.at[:, :, columns(g)],
            into.at[pl.ds(0, tiles_dev), inner_of(g, part)],
            (stock_sem.at[g], pool_sem.at[part])[target],
        )

    def moved(rows, size, sem):
        block = (pl.ds(0, rows), pl.ds(0, size * HEAD_DIM))
        return pltpu.make_async_copy(query_hbm.at[block], query_ref.at[block], sem)

    def sent(size, sem):
        block = query_ref.at[pl.ds(0, 2 * CAP * TILE), pl.ds(0, size * HEAD_DIM)]
        return remote(block, block, sem, swap_recv.at[0], other)

    def load_query():
        return pltpu.make_async_copy(query_hbm, query_ref, query_sem)

    for target in range(2):
        for g in range(count):
            load(g, 0, target).start()
            load(g, 1, target).start()
        if target == 0:
            load_query().start()

    for copy in tables:
        copy.wait()

    def entries(query_shard):
        first = jnp.clip(query_shard, 0, shards - 1) * tiles_dev
        found = []
        for row in range(tiles_dev):
            count = counts_ref[first + row]
            for pick in range(picks):
                found.append((select_ref[pick, first + row], pick < count))
        return found

    def span(found, owner):
        low, high = jnp.int32(tiles_dev), jnp.int32(-1)
        for tile, live in found:
            local = tile - owner * tiles_dev
            usable = (local >= 0) & (local < tiles_dev) & live
            low = jnp.where(usable, jnp.minimum(low, local), low)
            high = jnp.where(usable, jnp.maximum(high, local), high)
        return jnp.where(high < 0, 0, low), jnp.maximum(high, 0)

    for k in range(FLOWS):
        low, high = span(entries(shard + goes[k]), shard)
        send_ref[CAP * k] = low
        send_ref[CAP * k + 1] = high

    def remote(source, target, sent, landed, device):
        return pltpu.make_async_remote_copy(
            src_ref=source,
            dst_ref=target,
            send_sem=sent,
            recv_sem=landed,
            device_id={"seq": device},
            device_id_type=MESH,
        )

    def landing(g, piece, k):
        return pools[g][piece].at[pl.ds(tiles_dev + CAP * k, CAP)]

    def direct(g, piece, k):
        return remote(
            outgoing[g][piece].at[k],
            landing(g, piece, k),
            send_sem.at[k],
            recv_sem.at[units[g, piece]],
            index + 2 * goes[k],
        )

    def first_leg(g, piece, via):
        return remote(
            outgoing[g][piece].at[DIAG],
            relay[via][g][piece],
            send_sem.at[DIAG],
            relay_recv.at[units[g, piece], via],
            index + 2 * (-side, 2 * side)[via],
        )

    def second_leg(g, piece, via):
        return remote(
            relay[via][g][piece],
            landing(g, piece, DIAG),
            relay_send.at[via],
            recv_sem.at[units[g, piece]],
            index - 2 * (2 * side, side)[via],
        )

    def swap(g):
        return remote(
            away.at[:, columns(g)], theirs.at[:, columns(g)], swap_send, swap_recv.at[g], other
        )

    def gather(g):
        moved(query_ref.shape[0], 2 * groups[g][1], stock_sem.at[g]).wait()
        for p in range(len(pieces[g])):
            for k in range(FLOWS):
                for slot in range(CAP):
                    outgoing[g][p][k, slot] = stock[g][p][send_ref[CAP * k + slot]]

    def diagonal(g, act):
        if ladder:
            for via in range(2):

                @pl.when(takes(shard, g, via))
                def _(via=via):
                    for piece in range(len(pieces[g])):
                        act(first_leg(g, piece, via))

        else:

            @pl.when(inside(shard + side))
            def _():
                for piece in range(len(pieces[g])):
                    act(direct(g, piece, DIAG))

    def launch(g):
        if g + 1 < count:
            diagonal(g + 1, lambda copy: copy.start())
        for piece in range(len(pieces[g])):
            for k in (PAIR, UP, DOWN):

                @pl.when(inside(shard + goes[k]))
                def _(piece=piece, k=k):
                    direct(g, piece, k).start()

    def forward(g):
        for via in range(2 if ladder and g < count else 0):

            @pl.when(takes(shard - (side, 2 * side)[via], g, via))
            def _(via=via):
                for piece in range(len(pieces[g])):
                    first_leg(g, piece, via).wait_recv()
                    second_leg(g, piece, via).start()

    coming = jnp.int32(0)
    for offset in comes:
        coming = coming + jnp.where(inside(shard + offset), 1, 0)

    def arrive(g, piece):
        for flows in range(1, FLOWS + 1):

            @pl.when(coming == flows)
            def _(flows=flows):
                landed = pools[g][piece].at[pl.ds(tiles_dev, CAP * flows)]
                remote(
                    landed, landed, swap_send, recv_sem.at[units[g, piece]], other
                ).wait_recv()

    ahead = min(AHEAD, count)
    gather(0)
    pl.semaphore_wait(barrier, greeted)
    diagonal(0, lambda copy: copy.start())
    for g in range(min(ahead + 1, count)):
        if g + 1 < count:
            gather(g + 1)
        if g < ahead:
            launch(g)

    mine = entries(shard)
    lows = [span(mine, shard + comes[k])[0] for k in range(FLOWS)]
    for spot, (tile, live) in enumerate(mine):
        local = tile - shard * tiles_dev
        slot = jnp.where((local >= 0) & (local < tiles_dev), local, 0)
        for k in range(FLOWS):
            there = local - comes[k] * tiles_dev
            second = jnp.where(there == lows[k], 0, 1)
            slot = jnp.where(
                (there >= 0) & (there < tiles_dev), tiles_dev + CAP * k + second, slot
            )
        slots_ref[spot] = slot
        bias_ref[spot] = jnp.where(live, 0.0, -jnp.inf)

    load_query().wait()
    for part in range(2):
        moved(query_ref.shape[0], query_ref.shape[1] // HEAD_DIM, pool_sem.at[part]).wait()
    factor = HEAD_DIM**-0.5 * math.log2(math.e)

    def tile_of(g, part, slot, local):
        return pools[g][piece_of(g, part)][slot, inner_of(g, part), :, local]

    def slots_of(tile):
        return [slots_ref[tile * picks + p] for p in range(picks)]

    def weigh(g, tile, slots, local, cols):
        query = query_ref[pl.ds(pl.multiple_of(tile * TILE, TILE), TILE), cols]
        keys = jnp.concatenate([tile_of(g, 0, s, local) for s in slots], axis=0)
        scores = lax.dot_general(
            query, keys, (((1,), (1,)), ((), ())), preferred_element_type=jnp.float32
        )
        parts = [
            scores[:, p * TILE : (p + 1) * TILE] + bias_ref[tile * picks + p] for p in range(picks)
        ]
        top = jnp.max(functools.reduce(jnp.maximum, parts), axis=1, keepdims=True)
        weights = [jnp.exp2((part - top) * factor) for part in parts]
        total = jnp.sum(functools.reduce(jnp.add, weights), axis=1, keepdims=True)
        return jnp.concatenate([w.astype(jnp.bfloat16) for w in weights], axis=1), total

    def mix(g, slots, local, weights, total):
        values = jnp.concatenate([tile_of(g, 1, s, local) for s in slots], axis=0)
        mixed = jnp.dot(weights, values, preferred_element_type=jnp.float32)
        return (mixed / total).astype(jnp.bfloat16)

    def places(mine):
        which = half if mine else 1 - half
        for step in range(half_tiles):
            yield which * half_tiles + step, slice(step * TILE, (step + 1) * TILE)

    def attend(g, mine):
        first, size = groups[g]
        target = own if mine else away

        @pl.loop(0, size)
        def _(h):
            local = pl.ds(pl.multiple_of(h * HEAD_DIM, HEAD_DIM), HEAD_DIM)
            cols = pl.ds(pl.multiple_of((first + h) * HEAD_DIM, HEAD_DIM), HEAD_DIM)
            for tile, span_of in places(mine):
                slots = slots_of(tile)
                target[span_of, cols] = mix(g, slots, local, *weigh(g, tile, slots, local, cols))

    def attend_last(g):
        first, size = groups[g]
        spots = [(h, mine) for mine in (False, True) for h in range(size)]
        arrive(g, 0)
        totals = []
        for spot, (h, mine) in enumerate(spots):
            local = slice(h * HEAD_DIM, (h + 1) * HEAD_DIM)
            for step, (tile, _) in enumerate(places(mine)):
                cols = pl.ds((first + h) * HEAD_DIM, HEAD_DIM)
                weights, total = weigh(g, tile, slots_of(tile), local, cols)
                held[spot * half_tiles + step] = weights
                totals.append(total)
        arrive(g, 1)
        for spot, (h, mine) in enumerate(spots):
            local = slice(h * HEAD_DIM, (h + 1) * HEAD_DIM)
            for step, (tile, span_of) in enumerate(places(mine)):
                at = spot * half_tiles + step
                out = mix(g, slots_of(tile), local, held[at], totals[at])
                (own if mine else away)[span_of, pl.ds((first + h) * HEAD_DIM, HEAD_DIM)] = out
            if spot == size - 1:
                swap(g).start()

    def combine(g):
        swap(g).wait_recv()
        from_me = own[:, columns(g)].astype(jnp.float32)
        from_other = theirs[:, columns(g)].astype(jnp.float32)
        cond = jnp.where(half == 0, from_me, from_other)
        uncond = jnp.where(half == 0, from_other, from_me)
        out_ref[:, columns(g)] = (uncond + guide_ref[0] * (cond - uncond)).astype(jnp.bfloat16)

    forward(0)
    for g in range(count):
        forward(g + 1)
        if g + ahead + 2 < count:
            gather(g + ahead + 2)
        if g + ahead < count:
            launch(g + ahead)
        arrive(g, 0)
        attend(g, False)
        swap(g).start()
        attend(g, True)
        if g > 0:
            combine(g - 1)
    combine(count - 1)

    heads = query_ref.shape[1] // HEAD_DIM
    for k in range(FLOWS):

        @pl.when(inside(shard + goes[k]))
        def _(k=k):
            sent(heads, send_sem.at[k]).wait_send()

    for via in range(2 if ladder else 0):
        sender = shard - (side, 2 * side)[via]
        for part in range(planes):
            near = sum(groups[g][1] for g in near_groups(groups, part, planes))
            passed = (near, heads - near)[via]
            if passed:

                @pl.when(crosses(sender) & (share_of(sender) == part))
                def _(via=via, passed=passed):
                    sent(passed, relay_send.at[via]).wait_send()

    remote(away, theirs, swap_send, swap_recv.at[0], other).wait_send()


def pieces_of(groups):
    return [[(0, 1)]] * len(groups)


def unit_numbers(groups):
    return {
        unit: i
        for i, unit in enumerate(
            (g, p) for g, split in enumerate(pieces_of(groups)) for p in range(len(split))
        )
    }


def head_groups(heads):
    shares = GROUP_SHARES if heads == sum(GROUP_SHARES) else (1,) * heads
    groups, first = [], 0
    for share in shares:
        groups.append((first, share))
        first += share
    return groups


def body(ladder, query_rows, key_rows, value_rows, select, counts, guide_scale):
    tokens, width = query_rows.shape
    heads = width // HEAD_DIM
    tiles_dev = tokens // TILE
    picks = select.shape[1]
    half_rows = tokens // 2
    rows = jnp.bfloat16
    dma = pltpu.SemaphoreType.DMA
    hbm = pl.BlockSpec(memory_space=pl.ANY)
    groups = head_groups(heads)
    count, units = len(groups), len(unit_numbers(groups))
    half = pltpu.VMEM((half_rows, width), rows)

    def scratch(*lead):
        return [
            pltpu.VMEM((*lead, len(parts), TILE, size * HEAD_DIM), rows)
            for (_, size), split in zip(groups, pieces_of(groups), strict=True)
            for parts in split
        ]

    return pl.pallas_call(
        functools.partial(main_kernel, ladder, groups),
        out_shape=pltpu.VMEM((half_rows, width), rows),
        in_specs=[hbm, hbm, pl.BlockSpec(memory_space=SMEM), hbm, hbm, hbm],
        out_specs=pl.BlockSpec(memory_space=pltpu.VMEM),
        scratch_shapes=[
            *scratch(tiles_dev),
            *scratch(tiles_dev + CAP * FLOWS),
            *scratch(FLOWS, CAP),
            *scratch(CAP),
            *scratch(CAP),
            SMEM((picks, select.shape[0]), jnp.int32),
            SMEM(counts.shape, jnp.int32),
            pltpu.VMEM((tokens, width), rows),
            half,
            half,
            half,
            pltpu.VMEM((tiles_dev * groups[-1][1], TILE, picks * TILE), rows),
            SMEM((CAP * FLOWS,), jnp.int32),
            SMEM((tiles_dev * picks,), jnp.int32),
            SMEM((tiles_dev * picks,), jnp.float32),
            dma((count,)),
            dma((2,)),
            dma(()),
            dma((FLOWS,)),
            dma((units,)),
            dma((2,)),
            dma((units, 2)),
            dma(()),
            dma((count,)),
            dma((2,)),
        ],
        compiler_params=pltpu.CompilerParams(
            collective_id=0, has_side_effects=True, vmem_limit_bytes=60000 * 1024
        ),
        name="main",
    )(
        select.T,
        counts,
        guide_scale,
        query_rows,
        key_rows.reshape(tiles_dev, TILE, width),
        value_rows.reshape(tiles_dev, TILE, width),
    )


def is_ladder(mesh):
    devices = mesh.devices.reshape(mesh.shape["groups"], -1)[0][::2]
    places = [getattr(device, "coords", None) for device in devices]
    if any(place is None for place in places) or len(places) % 2:
        return False

    def hops(a, b):
        return sum(abs(p - q) for p, q in zip(places[a], places[b], strict=True))

    rungs = all(hops(s, s + 1) == 1 for s in range(0, len(places), 2))
    return rungs and all(hops(s, s + 2) == 1 for s in range(len(places) - 2))


def solution(mesh):
    in_specs = (
        P(("groups", "seq"), None),
        P(("groups", "seq"), None),
        P(("groups", "seq"), None),
        P("groups", None),
        P("groups"),
        P("groups"),
    )
    out_specs = P(("groups", "seq"), None)
    return jax.shard_map(
        functools.partial(body, is_ladder(mesh)),
        mesh=mesh,
        in_specs=in_specs,
        out_specs=out_specs,
        check_vma=False,
    )
```

```python
import functools
import itertools
import math

import jax
import jax.numpy as jnp
from jax import lax
from jax.experimental import pallas as pl
from jax.experimental.pallas import tpu as pltpu
from jax.sharding import PartitionSpec as P

HEAD_DIM = 128
TILE = 128
REACH = 2
CAP = 2
FLOWS = 4
PAIR, DIAG, UP, DOWN = range(FLOWS)
AHEAD = 2
LEAN = 0.25
GROUP_SHARES = (2, 2, 2, 2, 2, 1, 1)

SMEM = pltpu.SMEM
MESH = pl.DeviceIdType.MESH


def near_groups(groups, share, planes):
    chosen, owed = set(), 0.0
    for g, (_, size) in enumerate(groups):
        owed += share / planes * size
        if owed >= size / 2:
            chosen.add(g)
            owed -= size
    return chosen


def near_legs(groups, share, planes, more):
    sizes = {
        (g, leg): size * len(pieces_of(groups)[g][piece]) * slots / (2 * CAP)
        for g, (_, size) in enumerate(groups)
        for leg, (piece, _, slots) in enumerate(legs_of(groups)[g])
    }
    plain = {unit for unit in sizes if unit[0] in near_groups(groups, share, planes)}
    heads = sum(sizes.values())
    goal = sum(sizes[unit] for unit in plain) + more
    best, least = plain, None
    for bits in itertools.product((False, True), repeat=len(sizes)):
        chosen = {unit for unit, bit in zip(sizes, bits, strict=True) if bit}
        done, taken, drift = 0.0, 0.0, 0.0
        for unit, size in sizes.items():
            done, taken = done + size, taken + size * (unit in chosen)
            drift = max(drift, abs(taken - done * goal / heads))
        score = (abs(taken - goal), sum(sizes[unit] for unit in chosen ^ plain), drift)
        if least is None or score < least:
            best, least = chosen, score
    return best


def main_kernel(
    ladder,
    groups,
    select_hbm,
    counts_hbm,
    guide_ref,
    query_hbm,
    key_hbm,
    value_hbm,
    out_ref,
    *refs,
):
    count = len(groups)
    pieces = pieces_of(groups)
    units, legs, leg_numbers = numbers(pieces), legs_of(groups), numbers(legs_of(groups))
    refs = list(refs)
    stock, pools, outgoing, *relay = (
        [[refs.pop(0) for _ in pieces[g]] for g in range(count)] for _ in range(5)
    )
    select_ref, counts_ref, query_ref, own, away, theirs, held, *rest = refs
    send_ref, slots_ref, bias_ref, *sems = rest
    stock_sem, pool_sem, query_sem, send_sem, recv_sem, relay_send, relay_recv = sems[:7]
    swap_send, swap_recv, table_sem = sems[7:]
    picks = select_hbm.shape[0]
    tiles_dev = key_hbm.shape[0]
    half_tiles = tiles_dev // 2
    index = lax.axis_index("seq")
    shard, half = index // 2, index % 2
    shards = lax.axis_size("seq") // 2
    planes = shards // 2
    other = index + 1 - 2 * half
    side = 2 * (shard % 2) - 1
    goes = (-side, side, 2, -2)
    comes = (-side, side, -2, 2)

    def inside(place):
        return (place >= 0) & (place < shards)

    def share_of(sender):
        plane = sender // 2
        return jnp.where(sender % 2 == 1, planes - 1 - plane, plane)

    def crosses(sender):
        return inside(sender) & inside(sender + 2 * (sender % 2) - 1)

    near_by = {
        (odd, part): near_legs(groups, part, planes, LEAN * (1 - 2 * odd) * (part > 0))
        for odd in range(2)
        for part in range(planes if ladder else 0)
    }

    def takes(sender, g, leg, via):
        near = jnp.bool_(False)
        for (odd, part), chosen in near_by.items():
            if (g, leg) in chosen:
                near = near | ((share_of(sender) == part) & (sender % 2 == odd))
        return crosses(sender) & (near if via == 0 else jnp.logical_not(near))

    barrier = pltpu.get_barrier_semaphore()
    pl.semaphore_signal(barrier, inc=1, device_id={"seq": other}, device_id_type=MESH)
    greeted = jnp.int32(1)
    for offset in (-side, 2, -2) if ladder else goes:
        greeted = greeted + jnp.where(inside(shard + offset), 1, 0)

        @pl.when(inside(shard + offset))
        def _(offset=offset):
            pl.semaphore_signal(
                barrier, inc=1, device_id={"seq": index + 2 * offset}, device_id_type=MESH
            )

    tables = [
        pltpu.make_async_copy(source, target, table_sem.at[i])
        for i, (source, target) in enumerate(((select_hbm, select_ref), (counts_hbm, counts_ref)))
    ]
    for copy in tables:
        copy.start()

    def piece_of(g, part):
        return next(p for p, parts in enumerate(pieces[g]) if part in parts)

    def inner_of(g, part):
        return pieces[g][piece_of(g, part)].index(part)

    def columns(g):
        first, size = groups[g]
        return pl.ds(first * HEAD_DIM, size * HEAD_DIM)

    def load(g, part, target):
        source = (key_hbm, value_hbm)[part]
        into = (stock, pools)[target][g][piece_of(g, part)]
        return pltpu.make_async_copy(
            source.at[:, :, columns(g)],
            into.at[pl.ds(0, tiles_dev), inner_of(g, part)],
            (stock_sem.at[g], pool_sem.at[part])[target],
        )

    def moved(rows, size, sem):
        block = (pl.ds(0, rows), pl.ds(0, size * HEAD_DIM))
        return pltpu.make_async_copy(query_hbm.at[block], query_ref.at[block], sem)

    def sent(size, sem):
        block = query_ref.at[pl.ds(0, 2 * CAP * TILE), pl.ds(0, size * HEAD_DIM)]
        return remote(block, block, sem, swap_recv.at[0], other)

    def load_query():
        return pltpu.make_async_copy(query_hbm, query_ref, query_sem)

    for g in range(count):
        load(g, 0, 0).start()
        load(g, 1, 0).start()

    for copy in tables:
        copy.wait()

    def entries(query_shard):
        first = jnp.clip(query_shard, 0, shards - 1) * tiles_dev
        found = []
        for row in range(tiles_dev):
            count = counts_ref[first + row]
            for pick in range(picks):
                found.append((select_ref[pick, first + row], pick < count))
        return found

    def span(found, owner):
        low, high = jnp.int32(tiles_dev), jnp.int32(-1)
        for tile, live in found:
            local = tile - owner * tiles_dev
            usable = (local >= 0) & (local < tiles_dev) & live
            low = jnp.where(usable, jnp.minimum(low, local), low)
            high = jnp.where(usable, jnp.maximum(high, local), high)
        return jnp.where(high < 0, 0, low), jnp.maximum(high, 0)

    for k in range(FLOWS):
        low, high = span(entries(shard + goes[k]), shard)
        send_ref[CAP * k] = low
        send_ref[CAP * k + 1] = high

    def remote(source, target, sent, landed, device):
        return pltpu.make_async_remote_copy(
            src_ref=source,
            dst_ref=target,
            send_sem=sent,
            recv_sem=landed,
            device_id={"seq": device},
            device_id_type=MESH,
        )

    def landing(g, piece, k):
        return pools[g][piece].at[pl.ds(tiles_dev + CAP * k, CAP)]

    def direct(g, piece, k):
        return remote(
            outgoing[g][piece].at[k],
            landing(g, piece, k),
            send_sem.at[k],
            recv_sem.at[units[g, piece]],
            index + 2 * goes[k],
        )

    def first_leg(g, leg, via):
        piece, first, slots = legs[g][leg]
        return remote(
            outgoing[g][piece].at[DIAG, pl.ds(first, slots)],
            relay[via][g][piece].at[pl.ds(first, slots)],
            send_sem.at[DIAG],
            relay_recv.at[leg_numbers[g, leg], via],
            index + 2 * (-side, 2 * side)[via],
        )

    def second_leg(g, leg, via):
        piece, first, slots = legs[g][leg]
        return remote(
            relay[via][g][piece].at[pl.ds(first, slots)],
            pools[g][piece].at[pl.ds(tiles_dev + CAP * DIAG + first, slots)],
            relay_send.at[via, leg + 1 if g == count - 1 else 0],
            recv_sem.at[units[g, piece]],
            index - 2 * (2 * side, side)[via],
        )

    def swap(g):
        return remote(
            away.at[:, columns(g)], theirs.at[:, columns(g)], swap_send, swap_recv.at[g], other
        )

    def gather(g):
        moved(query_ref.shape[0], 2 * groups[g][1], stock_sem.at[g]).wait()
        for p in range(len(pieces[g])):
            for k in range(FLOWS):
                for slot in range(CAP):
                    outgoing[g][p][k, slot] = stock[g][p][send_ref[CAP * k + slot]]

    def diagonal(g, act):
        if ladder:
            for leg, via in itertools.product(range(len(legs[g])), range(2)):

                @pl.when(takes(shard, g, leg, via))
                def _(leg=leg, via=via):
                    act(first_leg(g, leg, via))

        else:

            @pl.when(inside(shard + side))
            def _():
                for piece in range(len(pieces[g])):
                    act(direct(g, piece, DIAG))

    def launch(g, diagonals=True, flows=(PAIR, UP, DOWN)):
        if g + 1 < count and diagonals:
            diagonal(g + 1, lambda copy: copy.start())
        for piece in range(len(pieces[g])):
            for k in flows:

                @pl.when(inside(shard + goes[k]))
                def _(piece=piece, k=k):
                    direct(g, piece, k).start()

    def forward(g):
        if not ladder or g >= count:
            return
        for leg, via in itertools.product(range(len(legs[g])), range(2)):

            @pl.when(takes(shard - (side, 2 * side)[via], g, leg, via))
            def _(leg=leg, via=via):
                first_leg(g, leg, via).wait_recv()
                second_leg(g, leg, via).start()

    coming = jnp.int32(0)
    for offset in comes:
        coming = coming + jnp.where(inside(shard + offset), 1, 0)

    def arrive(g, piece):
        for flows in range(1, FLOWS + 1):

            @pl.when(coming == flows)
            def _(flows=flows):
                landed = pools[g][piece].at[pl.ds(tiles_dev, CAP * flows)]
                remote(
                    landed, landed, swap_send, recv_sem.at[units[g, piece]], other
                ).wait_recv()

    ahead = min(AHEAD, count)
    gather(0)
    pl.semaphore_wait(barrier, greeted)
    diagonal(0, lambda copy: copy.start())
    launch(0, False, (UP, DOWN))
    for g in range(min(ahead + 1, count)):
        if g + 1 < count:
            gather(g + 1)
        if g < ahead:
            launch(g, True, (PAIR, UP, DOWN) if g else (PAIR,))
        if g == 0:
            load_query().start()
            for late in range(count):
                load(late, 0, 1).start()
                load(late, 1, 1).start()

    mine = entries(shard)
    lows = [span(mine, shard + comes[k])[0] for k in range(FLOWS)]
    for spot, (tile, live) in enumerate(mine):
        local = tile - shard * tiles_dev
        slot = jnp.where((local >= 0) & (local < tiles_dev), local, 0)
        for k in range(FLOWS):
            there = local - comes[k] * tiles_dev
            second = jnp.where(there == lows[k], 0, 1)
            slot = jnp.where(
                (there >= 0) & (there < tiles_dev), tiles_dev + CAP * k + second, slot
            )
        slots_ref[spot] = slot
        bias_ref[spot] = jnp.where(live, 0.0, -jnp.inf)

    load_query().wait()
    for part in range(2):
        moved(query_ref.shape[0], query_ref.shape[1] // HEAD_DIM, pool_sem.at[part]).wait()
    factor = HEAD_DIM**-0.5 * math.log2(math.e)

    def tile_of(g, part, slot, local):
        return pools[g][piece_of(g, part)][slot, inner_of(g, part), :, local]

    def slots_of(tile):
        return [slots_ref[tile * picks + p] for p in range(picks)]

    def weigh(g, tile, slots, local, cols):
        query = query_ref[pl.ds(pl.multiple_of(tile * TILE, TILE), TILE), cols]
        keys = jnp.concatenate([tile_of(g, 0, s, local) for s in slots], axis=0)
        scores = lax.dot_general(
            query, keys, (((1,), (1,)), ((), ())), preferred_element_type=jnp.float32
        )
        parts = [
            scores[:, p * TILE : (p + 1) * TILE] + bias_ref[tile * picks + p] for p in range(picks)
        ]
        top = jnp.max(functools.reduce(jnp.maximum, parts), axis=1, keepdims=True)
        weights = [jnp.exp2((part - top) * factor) for part in parts]
        total = jnp.sum(functools.reduce(jnp.add, weights), axis=1, keepdims=True)
        return jnp.concatenate([w.astype(jnp.bfloat16) for w in weights], axis=1), total

    def mix(g, slots, local, weights, total):
        values = jnp.concatenate([tile_of(g, 1, s, local) for s in slots], axis=0)
        mixed = jnp.dot(weights, values, preferred_element_type=jnp.float32)
        return (mixed / total).astype(jnp.bfloat16)

    def places(mine):
        which = half if mine else 1 - half
        for step in range(half_tiles):
            yield which * half_tiles + step, slice(step * TILE, (step + 1) * TILE)

    def attend(g, mine):
        first, size = groups[g]
        target = own if mine else away

        @pl.loop(0, size)
        def _(h):
            local = pl.ds(pl.multiple_of(h * HEAD_DIM, HEAD_DIM), HEAD_DIM)
            cols = pl.ds(pl.multiple_of((first + h) * HEAD_DIM, HEAD_DIM), HEAD_DIM)
            for tile, span_of in places(mine):
                slots = slots_of(tile)
                target[span_of, cols] = mix(g, slots, local, *weigh(g, tile, slots, local, cols))

    def attend_last(g):
        first, size = groups[g]
        spots = [(h, mine) for mine in (False, True) for h in range(size)]
        arrive(g, 0)
        totals = []
        for spot, (h, mine) in enumerate(spots):
            local = slice(h * HEAD_DIM, (h + 1) * HEAD_DIM)
            for step, (tile, _) in enumerate(places(mine)):
                cols = pl.ds((first + h) * HEAD_DIM, HEAD_DIM)
                weights, total = weigh(g, tile, slots_of(tile), local, cols)
                held[spot * half_tiles + step] = weights
                totals.append(total)
        arrive(g, 1)
        for spot, (h, mine) in enumerate(spots):
            local = slice(h * HEAD_DIM, (h + 1) * HEAD_DIM)
            for step, (tile, span_of) in enumerate(places(mine)):
                at = spot * half_tiles + step
                out = mix(g, slots_of(tile), local, held[at], totals[at])
                (own if mine else away)[span_of, pl.ds((first + h) * HEAD_DIM, HEAD_DIM)] = out
            if spot == size - 1:
                swap(g).start()

    def combine(g):
        swap(g).wait_recv()
        from_me = own[:, columns(g)].astype(jnp.float32)
        from_other = theirs[:, columns(g)].astype(jnp.float32)
        cond = jnp.where(half == 0, from_me, from_other)
        uncond = jnp.where(half == 0, from_other, from_me)
        out_ref[:, columns(g)] = (uncond + guide_ref[0] * (cond - uncond)).astype(jnp.bfloat16)

    forward(0)
    for g in range(count):
        if g == 0:
            forward(1)
        if g + ahead + 2 < count:
            gather(g + ahead + 2)
        if g + ahead < count:
            launch(g + ahead)
        if g < count - 1:
            arrive(g, 0)
            attend(g, False)
            swap(g).start()
            if g + 2 < count:
                forward(g + 2)
            attend(g, True)
        else:
            attend_last(g)
        if g > 0:
            combine(g - 1)
    combine(count - 1)

    heads = query_ref.shape[1] // HEAD_DIM
    for k in range(FLOWS):

        @pl.when(inside(shard + goes[k]))
        def _(k=k):
            sent(heads, send_sem.at[k]).wait_send()

    for via in range(2 if ladder else 0):
        sender = shard - (side, 2 * side)[via]
        for (odd, part), chosen in near_by.items():
            near = sum(groups[g][1] for g, _ in chosen if g < count - 1)
            passed = (near, heads - groups[-1][1] - near)[via]
            if passed:

                @pl.when(crosses(sender) & (share_of(sender) == part) & (sender % 2 == odd))
                def _(via=via, passed=passed):
                    sent(passed, relay_send.at[via, 0]).wait_send()

        for leg in range(len(legs[-1])):

            @pl.when(takes(sender, count - 1, leg, via))
            def _(via=via, leg=leg):
                second_leg(count - 1, leg, via).wait_send()

    remote(away, theirs, swap_send, swap_recv.at[0], other).wait_send()


def pieces_of(groups):
    return [[(0, 1)]] * (len(groups) - 1) + [[(0,), (1,)]]


def legs_of(groups):
    last = [(0, 0, CAP)] + [(1, slot, 1) for slot in range(CAP)]
    return [[(0, 0, CAP)]] * (len(groups) - 1) + [last]


def numbers(lists):
    pairs = ((g, i) for g, items in enumerate(lists) for i in range(len(items)))
    return {pair: number for number, pair in enumerate(pairs)}


def head_groups(heads):
    shares = GROUP_SHARES if heads == sum(GROUP_SHARES) else (1,) * heads
    groups, first = [], 0
    for share in shares:
        groups.append((first, share))
        first += share
    return groups


def body(ladder, query_rows, key_rows, value_rows, select, counts, guide_scale):
    tokens, width = query_rows.shape
    heads = width // HEAD_DIM
    tiles_dev = tokens // TILE
    picks = select.shape[1]
    half_rows = tokens // 2
    rows = jnp.bfloat16
    dma = pltpu.SemaphoreType.DMA
    hbm = pl.BlockSpec(memory_space=pl.ANY)
    groups = head_groups(heads)
    count, units = len(groups), len(numbers(pieces_of(groups)))
    legs = len(numbers(legs_of(groups)))
    half = pltpu.VMEM((half_rows, width), rows)

    def scratch(*lead):
        return [
            pltpu.VMEM((*lead, len(parts), TILE, size * HEAD_DIM), rows)
            for (_, size), split in zip(groups, pieces_of(groups), strict=True)
            for parts in split
        ]

    return pl.pallas_call(
        functools.partial(main_kernel, ladder, groups),
        out_shape=pltpu.VMEM((half_rows, width), rows),
        in_specs=[hbm, hbm, pl.BlockSpec(memory_space=SMEM), hbm, hbm, hbm],
        out_specs=pl.BlockSpec(memory_space=pltpu.VMEM),
        scratch_shapes=[
            *scratch(tiles_dev),
            *scratch(tiles_dev + CAP * FLOWS),
            *scratch(FLOWS, CAP),
            *scratch(CAP),
            *scratch(CAP),
            SMEM((picks, select.shape[0]), jnp.int32),
            SMEM(counts.shape, jnp.int32),
            pltpu.VMEM((tokens, width), rows),
            half,
            half,
            half,
            pltpu.VMEM((tiles_dev * groups[-1][1], TILE, picks * TILE), rows),
            SMEM((CAP * FLOWS,), jnp.int32),
            SMEM((tiles_dev * picks,), jnp.int32),
            SMEM((tiles_dev * picks,), jnp.float32),
            dma((count,)),
            dma((2,)),
            dma(()),
            dma((FLOWS,)),
            dma((units,)),
            dma((2, 1 + len(legs_of(groups)[-1]))),
            dma((legs, 2)),
            dma(()),
            dma((count,)),
            dma((2,)),
        ],
        compiler_params=pltpu.CompilerParams(
            collective_id=0, has_side_effects=True, vmem_limit_bytes=60000 * 1024
        ),
        name="main",
    )(
        select.T,
        counts,
        guide_scale,
        query_rows,
        key_rows.reshape(tiles_dev, TILE, width),
        value_rows.reshape(tiles_dev, TILE, width),
    )


def is_ladder(mesh):
    devices = mesh.devices.reshape(mesh.shape["groups"], -1)[0][::2]
    places = [getattr(device, "coords", None) for device in devices]
    if any(place is None for place in places) or len(places) % 2:
        return False

    def hops(a, b):
        return sum(abs(p - q) for p, q in zip(places[a], places[b], strict=True))

    rungs = all(hops(s, s + 1) == 1 for s in range(0, len(places), 2))
    return rungs and all(hops(s, s + 2) == 1 for s in range(len(places) - 2))


def solution(mesh):
    in_specs = (
        P(("groups", "seq"), None),
        P(("groups", "seq"), None),
        P(("groups", "seq"), None),
        P("groups", None),
        P("groups"),
        P("groups"),
    )
    out_specs = P(("groups", "seq"), None)
    return jax.shard_map(
        functools.partial(body, is_ladder(mesh)),
        mesh=mesh,
        in_specs=in_specs,
        out_specs=out_specs,
        check_vma=False,
    )
```

```python
import functools
import itertools
import math

import jax
import jax.numpy as jnp
from jax import lax
from jax.experimental import pallas as pl
from jax.experimental.pallas import tpu as pltpu
from jax.sharding import PartitionSpec as P

HEAD_DIM = 128
TILE = 128
REACH = 2
CAP = 2
FLOWS = 4
PAIR, DIAG, UP, DOWN = range(FLOWS)
AHEAD = 2
LEAN = 0.25
GROUP_SHARES = (2, 2, 2, 2, 2, 1, 1)

SMEM = pltpu.SMEM
MESH = pl.DeviceIdType.MESH


def near_groups(groups, share, planes):
    chosen, owed = set(), 0.0
    for g, (_, size) in enumerate(groups):
        owed += share / planes * size
        if owed >= size / 2:
            chosen.add(g)
            owed -= size
    return chosen


def near_legs(groups, share, planes, more):
    sizes = {
        (g, leg): size * len(pieces_of(groups)[g][piece]) * slots / (2 * CAP)
        for g, (_, size) in enumerate(groups)
        for leg, (piece, _, slots) in enumerate(legs_of(groups)[g])
    }
    plain = {unit for unit in sizes if unit[0] in near_groups(groups, share, planes)}
    heads = sum(sizes.values())
    goal = sum(sizes[unit] for unit in plain) + more
    best, least = plain, None
    for bits in itertools.product((False, True), repeat=len(sizes)):
        chosen = {unit for unit, bit in zip(sizes, bits, strict=True) if bit}
        done, taken, drift = 0.0, 0.0, 0.0
        for unit, size in sizes.items():
            done, taken = done + size, taken + size * (unit in chosen)
            drift = max(drift, abs(taken - done * goal / heads))
        score = (abs(taken - goal), sum(sizes[unit] for unit in chosen ^ plain), drift)
        if least is None or score < least:
            best, least = chosen, score
    return best


def main_kernel(
    ladder,
    groups,
    select_hbm,
    counts_hbm,
    guide_ref,
    query_hbm,
    key_hbm,
    value_hbm,
    out_ref,
    *refs,
):
    count = len(groups)
    pieces = pieces_of(groups)
    units, legs, leg_numbers = numbers(pieces), legs_of(groups), numbers(legs_of(groups))
    refs = list(refs)
    stock, pools, outgoing, *relay = (
        [[refs.pop(0) for _ in pieces[g]] for g in range(count)] for _ in range(5)
    )
    select_ref, counts_ref, query_ref, own, away, theirs, held, *rest = refs
    send_ref, slots_ref, bias_ref, *sems = rest
    stock_sem, pool_sem, query_sem, send_sem, recv_sem, relay_send, relay_recv = sems[:7]
    swap_send, swap_recv, table_sem = sems[7:]
    picks = select_hbm.shape[0]
    tiles_dev = key_hbm.shape[0]
    half_tiles = tiles_dev // 2
    index = lax.axis_index("seq")
    shard, half = index // 2, index % 2
    shards = lax.axis_size("seq") // 2
    planes = shards // 2
    other = index + 1 - 2 * half
    side = 2 * (shard % 2) - 1
    goes = (-side, side, 2, -2)
    comes = (-side, side, -2, 2)

    def inside(place):
        return (place >= 0) & (place < shards)

    def share_of(sender):
        plane = sender // 2
        return jnp.where(sender % 2 == 1, planes - 1 - plane, plane)

    def crosses(sender):
        return inside(sender) & inside(sender + 2 * (sender % 2) - 1)

    near_by = {
        (odd, part): near_legs(groups, part, planes, LEAN * (1 - 2 * odd) * (part > 0))
        for odd in range(2)
        for part in range(planes if ladder else 0)
    }

    def takes(sender, g, leg, via):
        near = jnp.bool_(False)
        for (odd, part), chosen in near_by.items():
            if (g, leg) in chosen:
                near = near | ((share_of(sender) == part) & (sender % 2 == odd))
        return crosses(sender) & (near if via == 0 else jnp.logical_not(near))

    barrier = pltpu.get_barrier_semaphore()
    pl.semaphore_signal(barrier, inc=1, device_id={"seq": other}, device_id_type=MESH)
    greeted = jnp.int32(1)
    for offset in (-side, 2, -2) if ladder else goes:
        greeted = greeted + jnp.where(inside(shard + offset), 1, 0)

        @pl.when(inside(shard + offset))
        def _(offset=offset):
            pl.semaphore_signal(
                barrier, inc=1, device_id={"seq": index + 2 * offset}, device_id_type=MESH
            )

    tables = [
        pltpu.make_async_copy(source, target, table_sem.at[i])
        for i, (source, target) in enumerate(((select_hbm, select_ref), (counts_hbm, counts_ref)))
    ]
    for copy in tables:
        copy.start()

    def piece_of(g, part):
        return next(p for p, parts in enumerate(pieces[g]) if part in parts)

    def inner_of(g, part):
        return pieces[g][piece_of(g, part)].index(part)

    def columns(g):
        first, size = groups[g]
        return pl.ds(first * HEAD_DIM, size * HEAD_DIM)

    def load(g, part, target):
        source = (key_hbm, value_hbm)[part]
        into = (stock, pools)[target][g][piece_of(g, part)]
        return pltpu.make_async_copy(
            source.at[:, :, columns(g)],
            into.at[pl.ds(0, tiles_dev), inner_of(g, part)],
            (stock_sem.at[g], pool_sem.at[part])[target],
        )

    def moved(rows, size, sem):
        block = (pl.ds(0, rows), pl.ds(0, size * HEAD_DIM))
        return pltpu.make_async_copy(query_hbm.at[block], query_ref.at[block], sem)

    def sent(size, sem):
        block = query_ref.at[pl.ds(0, 2 * CAP * TILE), pl.ds(0, size * HEAD_DIM)]
        return remote(block, block, sem, swap_recv.at[0], other)

    def load_query():
        return pltpu.make_async_copy(query_hbm, query_ref, query_sem)

    for g in range(count):
        load(g, 0, 0).start()
        load(g, 1, 0).start()

    for copy in tables:
        copy.wait()

    def entries(query_shard):
        first = jnp.clip(query_shard, 0, shards - 1) * tiles_dev
        found = []
        for row in range(tiles_dev):
            count = counts_ref[first + row]
            for pick in range(picks):
                found.append((select_ref[pick, first + row], pick < count))
        return found

    def span(found, owner):
        low, high = jnp.int32(tiles_dev), jnp.int32(-1)
        for tile, live in found:
            local = tile - owner * tiles_dev
            usable = (local >= 0) & (local < tiles_dev) & live
            low = jnp.where(usable, jnp.minimum(low, local), low)
            high = jnp.where(usable, jnp.maximum(high, local), high)
        return jnp.where(high < 0, 0, low), jnp.maximum(high, 0)

    for k in range(FLOWS):
        low, high = span(entries(shard + goes[k]), shard)
        send_ref[CAP * k] = low
        send_ref[CAP * k + 1] = high

    def remote(source, target, sent, landed, device):
        return pltpu.make_async_remote_copy(
            src_ref=source,
            dst_ref=target,
            send_sem=sent,
            recv_sem=landed,
            device_id={"seq": device},
            device_id_type=MESH,
        )

    def landing(g, piece, k):
        return pools[g][piece].at[pl.ds(tiles_dev + CAP * k, CAP)]

    def direct(g, piece, k):
        return remote(
            outgoing[g][piece].at[k],
            landing(g, piece, k),
            send_sem.at[k],
            recv_sem.at[units[g, piece]],
            index + 2 * goes[k],
        )

    def first_leg(g, leg, via):
        piece, first, slots = legs[g][leg]
        return remote(
            outgoing[g][piece].at[DIAG, pl.ds(first, slots)],
            relay[via][g][piece].at[pl.ds(first, slots)],
            send_sem.at[DIAG],
            relay_recv.at[leg_numbers[g, leg], via],
            index + 2 * (-side, 2 * side)[via],
        )

    def second_leg(g, leg, via):
        piece, first, slots = legs[g][leg]
        return remote(
            relay[via][g][piece].at[pl.ds(first, slots)],
            pools[g][piece].at[pl.ds(tiles_dev + CAP * DIAG + first, slots)],
            relay_send.at[via, leg + 1 if g == count - 1 else 0],
            recv_sem.at[units[g, piece]],
            index - 2 * (2 * side, side)[via],
        )

    def swap(g):
        return remote(
            away.at[:, columns(g)], theirs.at[:, columns(g)], swap_send, swap_recv.at[g], other
        )

    def gather(g):
        moved(query_ref.shape[0], 2 * groups[g][1], stock_sem.at[g]).wait()
        for p in range(len(pieces[g])):
            for k in range(FLOWS):
                for slot in range(CAP):
                    outgoing[g][p][k, slot] = stock[g][p][send_ref[CAP * k + slot]]

    def diagonal(g, act):
        if ladder:
            for leg, via in itertools.product(range(len(legs[g])), range(2)):

                @pl.when(takes(shard, g, leg, via))
                def _(leg=leg, via=via):
                    act(first_leg(g, leg, via))

        else:

            @pl.when(inside(shard + side))
            def _():
                for piece in range(len(pieces[g])):
                    act(direct(g, piece, DIAG))

    def launch(g, diagonals=True, flows=(PAIR, UP, DOWN)):
        if g + 1 < count and diagonals:
            diagonal(g + 1, lambda copy: copy.start())
        for piece in range(len(pieces[g])):
            for k in flows:

                @pl.when(inside(shard + goes[k]))
                def _(piece=piece, k=k):
                    direct(g, piece, k).start()

    def forward(g):
        if not ladder or g >= count:
            return
        for leg, via in itertools.product(range(len(legs[g])), range(2)):

            @pl.when(takes(shard - (side, 2 * side)[via], g, leg, via))
            def _(leg=leg, via=via):
                first_leg(g, leg, via).wait_recv()
                second_leg(g, leg, via).start()

    coming = jnp.int32(0)
    for offset in comes:
        coming = coming + jnp.where(inside(shard + offset), 1, 0)

    def arrive(g, piece):
        for flows in range(1, FLOWS + 1):

            @pl.when(coming == flows)
            def _(flows=flows):
                landed = pools[g][piece].at[pl.ds(tiles_dev, CAP * flows)]
                remote(
                    landed, landed, swap_send, recv_sem.at[units[g, piece]], other
                ).wait_recv()

    ahead = min(AHEAD, count)
    gather(0)
    pl.semaphore_wait(barrier, greeted)
    diagonal(0, lambda copy: copy.start())
    launch(0, False, (UP, DOWN))
    for g in range(min(ahead + 1, count)):
        if g + 1 < count:
            gather(g + 1)
        if g < ahead:
            launch(g, True, (PAIR, UP, DOWN) if g else (PAIR,))
        if g == 0:
            load_query().start()
            for late in range(count):
                load(late, 0, 1).start()
                load(late, 1, 1).start()

    mine = entries(shard)
    lows = [span(mine, shard + comes[k])[0] for k in range(FLOWS)]
    for spot, (tile, live) in enumerate(mine):
        local = tile - shard * tiles_dev
        slot = jnp.where((local >= 0) & (local < tiles_dev), local, 0)
        for k in range(FLOWS):
            there = local - comes[k] * tiles_dev
            second = jnp.where(there == lows[k], 0, 1)
            slot = jnp.where(
                (there >= 0) & (there < tiles_dev), tiles_dev + CAP * k + second, slot
            )
        slots_ref[spot] = slot
        bias_ref[spot] = jnp.where(live, 0.0, -jnp.inf)

    load_query().wait()
    for part in range(2):
        moved(query_ref.shape[0], query_ref.shape[1] // HEAD_DIM, pool_sem.at[part]).wait()
    factor = HEAD_DIM**-0.5 * math.log2(math.e)

    def tile_of(g, part, slot, local):
        return pools[g][piece_of(g, part)][slot, inner_of(g, part), :, local]

    def slots_of(tile):
        return [slots_ref[tile * picks + p] for p in range(picks)]

    def weigh(g, tile, slots, local, cols):
        query = query_ref[pl.ds(pl.multiple_of(tile * TILE, TILE), TILE), cols]
        keys = jnp.concatenate([tile_of(g, 0, s, local) for s in slots], axis=0)
        scores = lax.dot_general(
            query, keys, (((1,), (1,)), ((), ())), preferred_element_type=jnp.float32
        )
        parts = [
            scores[:, p * TILE : (p + 1) * TILE] + bias_ref[tile * picks + p] for p in range(picks)
        ]
        top = jnp.max(functools.reduce(jnp.maximum, parts), axis=1, keepdims=True)
        weights = [jnp.exp2((part - top) * factor) for part in parts]
        total = jnp.sum(functools.reduce(jnp.add, weights), axis=1, keepdims=True)
        return jnp.concatenate([w.astype(jnp.bfloat16) for w in weights], axis=1), total

    def mix(g, slots, local, weights, total):
        values = jnp.concatenate([tile_of(g, 1, s, local) for s in slots], axis=0)
        mixed = jnp.dot(weights, values, preferred_element_type=jnp.float32)
        return (mixed / total).astype(jnp.bfloat16)

    def places(mine):
        which = half if mine else 1 - half
        for step in range(half_tiles):
            yield which * half_tiles + step, slice(step * TILE, (step + 1) * TILE)

    def attend(g, mine):
        first, size = groups[g]
        target = own if mine else away

        @pl.loop(0, size)
        def _(h):
            local = pl.ds(pl.multiple_of(h * HEAD_DIM, HEAD_DIM), HEAD_DIM)
            cols = pl.ds(pl.multiple_of((first + h) * HEAD_DIM, HEAD_DIM), HEAD_DIM)
            for tile, span_of in places(mine):
                slots = slots_of(tile)
                target[span_of, cols] = mix(g, slots, local, *weigh(g, tile, slots, local, cols))

    def attend_last(g):
        first, size = groups[g]
        spots = [(h, mine) for mine in (False, True) for h in range(size)]
        arrive(g, 0)
        totals = []
        for spot, (h, mine) in enumerate(spots):
            local = slice(h * HEAD_DIM, (h + 1) * HEAD_DIM)
            for step, (tile, _) in enumerate(places(mine)):
                cols = pl.ds((first + h) * HEAD_DIM, HEAD_DIM)
                weights, total = weigh(g, tile, slots_of(tile), local, cols)
                held[spot * half_tiles + step] = weights
                totals.append(total)
        arrive(g, 1)
        for spot, (h, mine) in enumerate(spots):
            local = slice(h * HEAD_DIM, (h + 1) * HEAD_DIM)
            for step, (tile, span_of) in enumerate(places(mine)):
                at = spot * half_tiles + step
                out = mix(g, slots_of(tile), local, held[at], totals[at])
                (own if mine else away)[span_of, pl.ds((first + h) * HEAD_DIM, HEAD_DIM)] = out
            if spot == size - 1:
                swap(g).start()

    def combine(g):
        swap(g).wait_recv()
        from_me = own[:, columns(g)].astype(jnp.float32)
        from_other = theirs[:, columns(g)].astype(jnp.float32)
        cond = jnp.where(half == 0, from_me, from_other)
        uncond = jnp.where(half == 0, from_other, from_me)
        out_ref[:, columns(g)] = (uncond + guide_ref[0] * (cond - uncond)).astype(jnp.bfloat16)

    forward(0)
    for g in range(count):
        if g == 0:
            forward(1)
        if g + ahead < count:
            launch(g + ahead)
        if g < count - 1:
            arrive(g, 0)
            attend(g, False)
            swap(g).start()
            if g + 2 < count:
                forward(g + 2)
            if g + ahead + 2 < count:
                gather(g + ahead + 2)
            attend(g, True)
        else:
            attend_last(g)
        if g > 0:
            combine(g - 1)
    combine(count - 1)

    heads = query_ref.shape[1] // HEAD_DIM
    for k in range(FLOWS):

        @pl.when(inside(shard + goes[k]))
        def _(k=k):
            sent(heads, send_sem.at[k]).wait_send()

    for via in range(2 if ladder else 0):
        sender = shard - (side, 2 * side)[via]
        for (odd, part), chosen in near_by.items():
            near = sum(groups[g][1] for g, _ in chosen if g < count - 1)
            passed = (near, heads - groups[-1][1] - near)[via]
            if passed:

                @pl.when(crosses(sender) & (share_of(sender) == part) & (sender % 2 == odd))
                def _(via=via, passed=passed):
                    sent(passed, relay_send.at[via, 0]).wait_send()

        for leg in range(len(legs[-1])):

            @pl.when(takes(sender, count - 1, leg, via))
            def _(via=via, leg=leg):
                second_leg(count - 1, leg, via).wait_send()

    remote(away, theirs, swap_send, swap_recv.at[0], other).wait_send()


def pieces_of(groups):
    return [[(0, 1)]] * (len(groups) - 1) + [[(0,), (1,)]]


def legs_of(groups):
    last = [(0, 0, CAP)] + [(1, slot, 1) for slot in range(CAP)]
    return [[(0, 0, CAP)]] * (len(groups) - 1) + [last]


def numbers(lists):
    pairs = ((g, i) for g, items in enumerate(lists) for i in range(len(items)))
    return {pair: number for number, pair in enumerate(pairs)}


def head_groups(heads):
    shares = GROUP_SHARES if heads == sum(GROUP_SHARES) else (1,) * heads
    groups, first = [], 0
    for share in shares:
        groups.append((first, share))
        first += share
    return groups


def body(ladder, query_rows, key_rows, value_rows, select, counts, guide_scale):
    tokens, width = query_rows.shape
    heads = width // HEAD_DIM
    tiles_dev = tokens // TILE
    picks = select.shape[1]
    half_rows = tokens // 2
    rows = jnp.bfloat16
    dma = pltpu.SemaphoreType.DMA
    hbm = pl.BlockSpec(memory_space=pl.ANY)
    groups = head_groups(heads)
    count, units = len(groups), len(numbers(pieces_of(groups)))
    legs = len(numbers(legs_of(groups)))
    half = pltpu.VMEM((half_rows, width), rows)

    def scratch(*lead):
        return [
            pltpu.VMEM((*lead, len(parts), TILE, size * HEAD_DIM), rows)
            for (_, size), split in zip(groups, pieces_of(groups), strict=True)
            for parts in split
        ]

    return pl.pallas_call(
        functools.partial(main_kernel, ladder, groups),
        out_shape=pltpu.VMEM((half_rows, width), rows),
        in_specs=[hbm, hbm, pl.BlockSpec(memory_space=SMEM), hbm, hbm, hbm],
        out_specs=pl.BlockSpec(memory_space=pltpu.VMEM),
        scratch_shapes=[
            *scratch(tiles_dev),
            *scratch(tiles_dev + CAP * FLOWS),
            *scratch(FLOWS, CAP),
            *scratch(CAP),
            *scratch(CAP),
            SMEM((picks, select.shape[0]), jnp.int32),
            SMEM(counts.shape, jnp.int32),
            pltpu.VMEM((tokens, width), rows),
            half,
            half,
            half,
            pltpu.VMEM((tiles_dev * groups[-1][1], TILE, picks * TILE), rows),
            SMEM((CAP * FLOWS,), jnp.int32),
            SMEM((tiles_dev * picks,), jnp.int32),
            SMEM((tiles_dev * picks,), jnp.float32),
            dma((count,)),
            dma((2,)),
            dma(()),
            dma((FLOWS,)),
            dma((units,)),
            dma((2, 1 + len(legs_of(groups)[-1]))),
            dma((legs, 2)),
            dma(()),
            dma((count,)),
            dma((2,)),
        ],
        compiler_params=pltpu.CompilerParams(
            collective_id=0, has_side_effects=True, vmem_limit_bytes=60000 * 1024
        ),
        name="main",
    )(
        select.T,
        counts,
        guide_scale,
        query_rows,
        key_rows.reshape(tiles_dev, TILE, width),
        value_rows.reshape(tiles_dev, TILE, width),
    )


def is_ladder(mesh):
    devices = mesh.devices.reshape(mesh.shape["groups"], -1)[0][::2]
    places = [getattr(device, "coords", None) for device in devices]
    if any(place is None for place in places) or len(places) % 2:
        return False

    def hops(a, b):
        return sum(abs(p - q) for p, q in zip(places[a], places[b], strict=True))

    rungs = all(hops(s, s + 1) == 1 for s in range(0, len(places), 2))
    return rungs and all(hops(s, s + 2) == 1 for s in range(len(places) - 2))


def solution(mesh):
    in_specs = (
        P(("groups", "seq"), None),
        P(("groups", "seq"), None),
        P(("groups", "seq"), None),
        P("groups", None),
        P("groups"),
        P("groups"),
    )
    out_specs = P(("groups", "seq"), None)
    return jax.shard_map(
        functools.partial(body, is_ladder(mesh)),
        mesh=mesh,
        in_specs=in_specs,
        out_specs=out_specs,
        check_vma=False,
    )
```

```python
import functools
import itertools
import math

import jax
import jax.numpy as jnp
from jax import lax
from jax.experimental import pallas as pl
from jax.experimental.pallas import tpu as pltpu
from jax.sharding import PartitionSpec as P

HEAD_DIM = 128
TILE = 128
REACH = 2
CAP = 2
FLOWS = 4
PAIR, DIAG, UP, DOWN = range(FLOWS)
AHEAD = 2
LEAN = 0.25
GROUP_SHARES = (2, 2, 2, 2, 2, 1, 1)

SMEM = pltpu.SMEM
MESH = pl.DeviceIdType.MESH


def near_groups(groups, share, planes):
    chosen, owed = set(), 0.0
    for g, (_, size) in enumerate(groups):
        owed += share / planes * size
        if owed >= size / 2:
            chosen.add(g)
            owed -= size
    return chosen


def near_legs(groups, share, planes, more):
    sizes = {
        (g, leg): size * len(pieces_of(groups)[g][piece]) * slots / (2 * CAP)
        for g, (_, size) in enumerate(groups)
        for leg, (piece, _, slots) in enumerate(legs_of(groups)[g])
    }
    plain = {unit for unit in sizes if unit[0] in near_groups(groups, share, planes)}
    heads = sum(sizes.values())
    goal = sum(sizes[unit] for unit in plain) + more
    best, least = plain, None
    for bits in itertools.product((False, True), repeat=len(sizes)):
        chosen = {unit for unit, bit in zip(sizes, bits, strict=True) if bit}
        done, taken, drift = 0.0, 0.0, 0.0
        for unit, size in sizes.items():
            done, taken = done + size, taken + size * (unit in chosen)
            drift = max(drift, abs(taken - done * goal / heads))
        score = (abs(taken - goal), sum(sizes[unit] for unit in chosen ^ plain), drift)
        if least is None or score < least:
            best, least = chosen, score
    return best


def main_kernel(
    ladder,
    groups,
    select_hbm,
    counts_hbm,
    guide_ref,
    query_hbm,
    key_hbm,
    value_hbm,
    out_ref,
    *refs,
):
    count = len(groups)
    pieces = pieces_of(groups)
    units, legs, leg_numbers = numbers(pieces), legs_of(groups), numbers(legs_of(groups))
    refs = list(refs)
    stock, pools, outgoing, *relay = (
        [[refs.pop(0) for _ in pieces[g]] for g in range(count)] for _ in range(5)
    )
    select_ref, counts_ref, query_ref, own, away, theirs, held, *rest = refs
    send_ref, slots_ref, bias_ref, *sems = rest
    stock_sem, pool_sem, query_sem, send_sem, recv_sem, relay_send, relay_recv = sems[:7]
    swap_send, swap_recv, table_sem = sems[7:]
    picks = select_hbm.shape[0]
    tiles_dev = key_hbm.shape[0]
    half_tiles = tiles_dev // 2
    index = lax.axis_index("seq")
    shard, half = index // 2, index % 2
    shards = lax.axis_size("seq") // 2
    planes = shards // 2
    other = index + 1 - 2 * half
    side = 2 * (shard % 2) - 1
    goes = (-side, side, 2, -2)
    comes = (-side, side, -2, 2)

    def inside(place):
        return (place >= 0) & (place < shards)

    def share_of(sender):
        plane = sender // 2
        return jnp.where(sender % 2 == 1, planes - 1 - plane, plane)

    def crosses(sender):
        return inside(sender) & inside(sender + 2 * (sender % 2) - 1)

    near_by = {
        (odd, part): near_legs(groups, part, planes, LEAN * (1 - 2 * odd) * (part > 0))
        for odd in range(2)
        for part in range(planes if ladder else 0)
    }

    def takes(sender, g, leg, via):
        near = jnp.bool_(False)
        for (odd, part), chosen in near_by.items():
            if (g, leg) in chosen:
                near = near | ((share_of(sender) == part) & (sender % 2 == odd))
        return crosses(sender) & (near if via == 0 else jnp.logical_not(near))

    barrier = pltpu.get_barrier_semaphore()
    pl.semaphore_signal(barrier, inc=1, device_id={"seq": other}, device_id_type=MESH)
    greeted = jnp.int32(1)
    for offset in (-side, 2, -2) if ladder else goes:
        greeted = greeted + jnp.where(inside(shard + offset), 1, 0)

        @pl.when(inside(shard + offset))
        def _(offset=offset):
            pl.semaphore_signal(
                barrier, inc=1, device_id={"seq": index + 2 * offset}, device_id_type=MESH
            )

    tables = [
        pltpu.make_async_copy(source, target, table_sem.at[i])
        for i, (source, target) in enumerate(((select_hbm, select_ref), (counts_hbm, counts_ref)))
    ]
    for copy in tables:
        copy.start()

    def piece_of(g, part):
        return next(p for p, parts in enumerate(pieces[g]) if part in parts)

    def inner_of(g, part):
        return pieces[g][piece_of(g, part)].index(part)

    def columns(g):
        first, size = groups[g]
        return pl.ds(first * HEAD_DIM, size * HEAD_DIM)

    def load(g, part, target):
        source = (key_hbm, value_hbm)[part]
        into = (stock, pools)[target][g][piece_of(g, part)]
        return pltpu.make_async_copy(
            source.at[:, :, columns(g)],
            into.at[pl.ds(0, tiles_dev), inner_of(g, part)],
            (stock_sem.at[g], pool_sem.at[part])[target],
        )

    def moved(rows, size, sem):
        block = (pl.ds(0, rows), pl.ds(0, size * HEAD_DIM))
        return pltpu.make_async_copy(query_hbm.at[block], query_ref.at[block], sem)

    def sent(size, sem):
        block = query_ref.at[pl.ds(0, 2 * CAP * TILE), pl.ds(0, size * HEAD_DIM)]
        return remote(block, block, sem, swap_recv.at[0], other)

    def load_query():
        return pltpu.make_async_copy(query_hbm, query_ref, query_sem)

    for g in range(count):
        load(g, 0, 0).start()
        load(g, 1, 0).start()

    for copy in tables:
        copy.wait()

    def entries(query_shard):
        first = jnp.clip(query_shard, 0, shards - 1) * tiles_dev
        found = []
        for row in range(tiles_dev):
            count = counts_ref[first + row]
            for pick in range(picks):
                found.append((select_ref[pick, first + row], pick < count))
        return found

    def span(found, owner):
        low, high = jnp.int32(tiles_dev), jnp.int32(-1)
        for tile, live in found:
            local = tile - owner * tiles_dev
            usable = (local >= 0) & (local < tiles_dev) & live
            low = jnp.where(usable, jnp.minimum(low, local), low)
            high = jnp.where(usable, jnp.maximum(high, local), high)
        return jnp.where(high < 0, 0, low), jnp.maximum(high, 0)

    for k in range(FLOWS):
        low, high = span(entries(shard + goes[k]), shard)
        send_ref[CAP * k] = low
        send_ref[CAP * k + 1] = high

    def remote(source, target, sent, landed, device):
        return pltpu.make_async_remote_copy(
            src_ref=source,
            dst_ref=target,
            send_sem=sent,
            recv_sem=landed,
            device_id={"seq": device},
            device_id_type=MESH,
        )

    def landing(g, piece, k):
        return pools[g][piece].at[pl.ds(tiles_dev + CAP * k, CAP)]

    def direct(g, piece, k):
        return remote(
            outgoing[g][piece].at[k],
            landing(g, piece, k),
            send_sem.at[k],
            recv_sem.at[units[g, piece]],
            index + 2 * goes[k],
        )

    def first_leg(g, leg, via):
        piece, first, slots = legs[g][leg]
        return remote(
            outgoing[g][piece].at[DIAG, pl.ds(first, slots)],
            relay[via][g][piece].at[pl.ds(first, slots)],
            send_sem.at[DIAG],
            relay_recv.at[leg_numbers[g, leg], via],
            index + 2 * (-side, 2 * side)[via],
        )

    def second_leg(g, leg, via):
        piece, first, slots = legs[g][leg]
        return remote(
            relay[via][g][piece].at[pl.ds(first, slots)],
            pools[g][piece].at[pl.ds(tiles_dev + CAP * DIAG + first, slots)],
            relay_send.at[via, leg + 1 if g == count - 1 else 0],
            recv_sem.at[units[g, piece]],
            index - 2 * (2 * side, side)[via],
        )

    def swap(g):
        return remote(
            away.at[:, columns(g)], theirs.at[:, columns(g)], swap_send, swap_recv.at[g], other
        )

    def gather(g):
        moved(query_ref.shape[0], 2 * groups[g][1], stock_sem.at[g]).wait()
        for p in range(len(pieces[g])):
            for k in range(FLOWS):
                for slot in range(CAP):
                    outgoing[g][p][k, slot] = stock[g][p][send_ref[CAP * k + slot]]

    def diagonal(g, act):
        if ladder:
            for leg, via in itertools.product(range(len(legs[g])), range(2)):

                @pl.when(takes(shard, g, leg, via))
                def _(leg=leg, via=via):
                    act(first_leg(g, leg, via))

        else:

            @pl.when(inside(shard + side))
            def _():
                for piece in range(len(pieces[g])):
                    act(direct(g, piece, DIAG))

    def launch(g, diagonals=True, flows=(PAIR, UP, DOWN)):
        if g + 1 < count and diagonals:
            diagonal(g + 1, lambda copy: copy.start())
        for piece in range(len(pieces[g])):
            for k in flows:

                @pl.when(inside(shard + goes[k]))
                def _(piece=piece, k=k):
                    direct(g, piece, k).start()

    def forward(g):
        if not ladder or g >= count:
            return
        for leg, via in itertools.product(range(len(legs[g])), range(2)):

            @pl.when(takes(shard - (side, 2 * side)[via], g, leg, via))
            def _(leg=leg, via=via):
                first_leg(g, leg, via).wait_recv()
                second_leg(g, leg, via).start()

    coming = jnp.int32(0)
    for offset in comes:
        coming = coming + jnp.where(inside(shard + offset), 1, 0)

    def arrive(g, piece):
        for flows in range(1, FLOWS + 1):

            @pl.when(coming == flows)
            def _(flows=flows):
                landed = pools[g][piece].at[pl.ds(tiles_dev, CAP * flows)]
                remote(
                    landed, landed, swap_send, recv_sem.at[units[g, piece]], other
                ).wait_recv()

    ahead = min(AHEAD, count)
    gather(0)
    pl.semaphore_wait(barrier, greeted)
    diagonal(0, lambda copy: copy.start())
    launch(0, False, (UP, DOWN))
    for g in range(min(ahead + 1, count)):
        if g + 1 < count:
            gather(g + 1)
        if g < ahead:
            launch(g, True, (PAIR, UP, DOWN) if g else (PAIR,))
        if g == 0:
            load_query().start()
            for late in range(count):
                load(late, 0, 1).start()
                load(late, 1, 1).start()

    mine = entries(shard)
    lows = [span(mine, shard + comes[k])[0] for k in range(FLOWS)]
    for spot, (tile, live) in enumerate(mine):
        local = tile - shard * tiles_dev
        slot = jnp.where((local >= 0) & (local < tiles_dev), local, 0)
        for k in range(FLOWS):
            there = local - comes[k] * tiles_dev
            second = jnp.where(there == lows[k], 0, 1)
            slot = jnp.where(
                (there >= 0) & (there < tiles_dev), tiles_dev + CAP * k + second, slot
            )
        slots_ref[spot] = slot
        bias_ref[spot] = jnp.where(live, 0.0, -jnp.inf)

    load_query().wait()
    for part in range(2):
        moved(query_ref.shape[0], query_ref.shape[1] // HEAD_DIM, pool_sem.at[part]).wait()
    factor = HEAD_DIM**-0.5 * math.log2(math.e)

    def tile_of(g, part, slot, local):
        return pools[g][piece_of(g, part)][slot, inner_of(g, part), :, local]

    def slots_of(tile):
        return [slots_ref[tile * picks + p] for p in range(picks)]

    def weigh(g, tile, slots, local, cols):
        query = query_ref[pl.ds(pl.multiple_of(tile * TILE, TILE), TILE), cols]
        keys = jnp.concatenate([tile_of(g, 0, s, local) for s in slots], axis=0)
        scores = lax.dot_general(
            query, keys, (((1,), (1,)), ((), ())), preferred_element_type=jnp.float32
        )
        parts = [
            scores[:, p * TILE : (p + 1) * TILE] + bias_ref[tile * picks + p] for p in range(picks)
        ]
        top = jnp.max(functools.reduce(jnp.maximum, parts), axis=1, keepdims=True)
        weights = [jnp.exp2((part - top) * factor) for part in parts]
        total = jnp.sum(functools.reduce(jnp.add, weights), axis=1, keepdims=True)
        return jnp.concatenate([w.astype(jnp.bfloat16) for w in weights], axis=1), total

    def mix(g, slots, local, weights, total):
        values = jnp.concatenate([tile_of(g, 1, s, local) for s in slots], axis=0)
        mixed = jnp.dot(weights, values, preferred_element_type=jnp.float32)
        return (mixed / total).astype(jnp.bfloat16)

    def places(mine):
        which = half if mine else 1 - half
        for step in range(half_tiles):
            yield which * half_tiles + step, slice(step * TILE, (step + 1) * TILE)

    def attend(g, mine):
        first, size = groups[g]
        target = own if mine else away

        @pl.loop(0, size)
        def _(h):
            local = pl.ds(pl.multiple_of(h * HEAD_DIM, HEAD_DIM), HEAD_DIM)
            cols = pl.ds(pl.multiple_of((first + h) * HEAD_DIM, HEAD_DIM), HEAD_DIM)
            for tile, span_of in places(mine):
                slots = slots_of(tile)
                target[span_of, cols] = mix(g, slots, local, *weigh(g, tile, slots, local, cols))

    def attend_last(g):
        first, size = groups[g]
        spots = [(h, mine) for mine in (False, True) for h in range(size)]
        arrive(g, 0)
        totals = []
        for spot, (h, mine) in enumerate(spots):
            local = slice(h * HEAD_DIM, (h + 1) * HEAD_DIM)
            for step, (tile, _) in enumerate(places(mine)):
                cols = pl.ds((first + h) * HEAD_DIM, HEAD_DIM)
                weights, total = weigh(g, tile, slots_of(tile), local, cols)
                held[spot * half_tiles + step] = weights
                totals.append(total)
        arrive(g, 1)
        for spot, (h, mine) in enumerate(spots):
            local = slice(h * HEAD_DIM, (h + 1) * HEAD_DIM)
            for step, (tile, span_of) in enumerate(places(mine)):
                at = spot * half_tiles + step
                out = mix(g, slots_of(tile), local, held[at], totals[at])
                cols = pl.ds((first + h) * HEAD_DIM, HEAD_DIM)
                (own if mine else away)[span_of, cols] = out
                if not mine:
                    block = (pl.ds(step * TILE, TILE), cols)
                    remote(
                        away.at[block], theirs.at[block], swap_send, swap_recv.at[g], other
                    ).start()

    def combine(g):
        swap(g).wait_recv()
        from_me = own[:, columns(g)].astype(jnp.float32)
        from_other = theirs[:, columns(g)].astype(jnp.float32)
        cond = jnp.where(half == 0, from_me, from_other)
        uncond = jnp.where(half == 0, from_other, from_me)
        out_ref[:, columns(g)] = (uncond + guide_ref[0] * (cond - uncond)).astype(jnp.bfloat16)

    forward(0)
    for g in range(count):
        if g == 0:
            forward(1)
        if g + ahead < count:
            launch(g + ahead)
        if g < count - 1:
            arrive(g, 0)
            attend(g, False)
            swap(g).start()
            if g + 2 < count:
                forward(g + 2)
            if g + ahead + 2 < count:
                gather(g + ahead + 2)
            attend(g, True)
        else:
            attend_last(g)
        if g > 0:
            combine(g - 1)
    combine(count - 1)

    heads = query_ref.shape[1] // HEAD_DIM
    for k in range(FLOWS):

        @pl.when(inside(shard + goes[k]))
        def _(k=k):
            sent(heads, send_sem.at[k]).wait_send()

    for via in range(2 if ladder else 0):
        sender = shard - (side, 2 * side)[via]
        for (odd, part), chosen in near_by.items():
            near = sum(groups[g][1] for g, _ in chosen if g < count - 1)
            passed = (near, heads - groups[-1][1] - near)[via]
            if passed:

                @pl.when(crosses(sender) & (share_of(sender) == part) & (sender % 2 == odd))
                def _(via=via, passed=passed):
                    sent(passed, relay_send.at[via, 0]).wait_send()

        for leg in range(len(legs[-1])):

            @pl.when(takes(sender, count - 1, leg, via))
            def _(via=via, leg=leg):
                second_leg(count - 1, leg, via).wait_send()

    remote(away, theirs, swap_send, swap_recv.at[0], other).wait_send()


def pieces_of(groups):
    return [[(0, 1)]] * (len(groups) - 1) + [[(0,), (1,)]]


def legs_of(groups):
    last = [(0, 0, CAP)] + [(1, slot, 1) for slot in range(CAP)]
    return [[(0, 0, CAP)]] * (len(groups) - 1) + [last]


def numbers(lists):
    pairs = ((g, i) for g, items in enumerate(lists) for i in range(len(items)))
    return {pair: number for number, pair in enumerate(pairs)}


def head_groups(heads):
    shares = GROUP_SHARES if heads == sum(GROUP_SHARES) else (1,) * heads
    groups, first = [], 0
    for share in shares:
        groups.append((first, share))
        first += share
    return groups


def body(ladder, query_rows, key_rows, value_rows, select, counts, guide_scale):
    tokens, width = query_rows.shape
    heads = width // HEAD_DIM
    tiles_dev = tokens // TILE
    picks = select.shape[1]
    half_rows = tokens // 2
    rows = jnp.bfloat16
    dma = pltpu.SemaphoreType.DMA
    hbm = pl.BlockSpec(memory_space=pl.ANY)
    groups = head_groups(heads)
    count, units = len(groups), len(numbers(pieces_of(groups)))
    legs = len(numbers(legs_of(groups)))
    half = pltpu.VMEM((half_rows, width), rows)

    def scratch(*lead):
        return [
            pltpu.VMEM((*lead, len(parts), TILE, size * HEAD_DIM), rows)
            for (_, size), split in zip(groups, pieces_of(groups), strict=True)
            for parts in split
        ]

    return pl.pallas_call(
        functools.partial(main_kernel, ladder, groups),
        out_shape=pltpu.VMEM((half_rows, width), rows),
        in_specs=[hbm, hbm, pl.BlockSpec(memory_space=SMEM), hbm, hbm, hbm],
        out_specs=pl.BlockSpec(memory_space=pltpu.VMEM),
        scratch_shapes=[
            *scratch(tiles_dev),
            *scratch(tiles_dev + CAP * FLOWS),
            *scratch(FLOWS, CAP),
            *scratch(CAP),
            *scratch(CAP),
            SMEM((picks, select.shape[0]), jnp.int32),
            SMEM(counts.shape, jnp.int32),
            pltpu.VMEM((tokens, width), rows),
            half,
            half,
            half,
            pltpu.VMEM((tiles_dev * groups[-1][1], TILE, picks * TILE), rows),
            SMEM((CAP * FLOWS,), jnp.int32),
            SMEM((tiles_dev * picks,), jnp.int32),
            SMEM((tiles_dev * picks,), jnp.float32),
            dma((count,)),
            dma((2,)),
            dma(()),
            dma((FLOWS,)),
            dma((units,)),
            dma((2, 1 + len(legs_of(groups)[-1]))),
            dma((legs, 2)),
            dma(()),
            dma((count,)),
            dma((2,)),
        ],
        compiler_params=pltpu.CompilerParams(
            collective_id=0, has_side_effects=True, vmem_limit_bytes=60000 * 1024
        ),
        name="main",
    )(
        select.T,
        counts,
        guide_scale,
        query_rows,
        key_rows.reshape(tiles_dev, TILE, width),
        value_rows.reshape(tiles_dev, TILE, width),
    )


def is_ladder(mesh):
    devices = mesh.devices.reshape(mesh.shape["groups"], -1)[0][::2]
    places = [getattr(device, "coords", None) for device in devices]
    if any(place is None for place in places) or len(places) % 2:
        return False

    def hops(a, b):
        return sum(abs(p - q) for p, q in zip(places[a], places[b], strict=True))

    rungs = all(hops(s, s + 1) == 1 for s in range(0, len(places), 2))
    return rungs and all(hops(s, s + 2) == 1 for s in range(len(places) - 2))


def solution(mesh):
    in_specs = (
        P(("groups", "seq"), None),
        P(("groups", "seq"), None),
        P(("groups", "seq"), None),
        P("groups", None),
        P("groups"),
        P("groups"),
    )
    out_specs = P(("groups", "seq"), None)
    return jax.shard_map(
        functools.partial(body, is_ladder(mesh)),
        mesh=mesh,
        in_specs=in_specs,
        out_specs=out_specs,
        check_vma=False,
    )
```
